16 devices in a mesh: dp: 2 (over z), vp: 8 (over y, x, core).
Axes of the slice: x: 2, y: 2, z: 2, core: 2. Of those that a mesh axis runs over, the one named last changes fastest.
Arguments:
- hidden: bfloat16 [6, 256, 1024], P('dp')
- norm_gain: float32 [1024], replicated
- emb_table: bfloat16 [151936, 1024], P('vp')
- labels: int32 [6, 256], P('dp')
- tok_mask: float32 [6, 256], P('dp')
Outputs:
- output 1: float32 [], replicated
- output 2: float32 [151936, 1024], P('vp')
- output 3: bfloat16 [6, 256, 1024], P('dp')
- output 4: float32 [1024], replicated
All inputs are finite; a program needn't handle non-finite values.
Results may differ from the reference program's by a relative error of at most 0.001.
Values sent between devices are 32-bit elements.
A program may use at most 1 GiB of HBM per device.

```python
import math
import jax
import jax.numpy as jnp
from jax import lax

WIDTH = 1024
VOCAB = 151936
BATCH = 6
SEQ_LEN = 256
LOGIT_SCALE = 0.0625
EPS = 1e-5
EMB_GAIN = 48.0
TARGET_PULL = 4.0
BLOCK_ROWS = math.gcd(BATCH, max(1, 2**25 // (SEQ_LEN * VOCAB)))
NUM_BLOCKS = BATCH // BLOCK_ROWS
BLOCK_TOKENS = BLOCK_ROWS * SEQ_LEN


def setup_inputs(seed: int = 0) -> dict:
    key = jax.random.key(seed)
    key_table, key_noise, key_gain, key_labels, key_lengths = jax.random.split(key, 5)
    emb_std = EMB_GAIN / math.sqrt(WIDTH)
    emb_table = (jax.random.normal(key_table, (VOCAB, WIDTH), jnp.float32) * emb_std).astype(jnp.bfloat16)
    labels = jax.random.randint(key_labels, (BATCH, SEQ_LEN), 0, VOCAB, dtype=jnp.int32)
    target_rows = jnp.take(emb_table, labels, axis=0).astype(jnp.float32) / emb_std
    noise = jax.random.normal(key_noise, (BATCH, SEQ_LEN, WIDTH), jnp.float32)
    hidden = (noise + (TARGET_PULL / math.sqrt(WIDTH)) * target_rows).astype(jnp.bfloat16)
    lengths = jax.random.randint(key_lengths, (BATCH, 1), max(1, SEQ_LEN // 4), SEQ_LEN + 1, dtype=jnp.int32)
    tok_mask = (jnp.arange(SEQ_LEN)[None, :] < lengths).astype(jnp.float32)
    norm_gain = 1.0 + 0.25 * jax.random.normal(key_gain, (WIDTH,), jnp.float32)
    return {'hidden': hidden, 'norm_gain': norm_gain, 'emb_table': emb_table, 'labels': labels, 'tok_mask': tok_mask}


def norm_forward(tokens, norm_gain):
    values = tokens.astype(jnp.float32)
    mean_x = jnp.mean(values, axis=-1, keepdims=True)
    centered = values - mean_x
    variance = jnp.mean(centered * centered, axis=-1, keepdims=True)
    inv_std = lax.rsqrt(variance + EPS)
    x_hat = centered * inv_std
    return (norm_gain * x_hat).astype(jnp.bfloat16), x_hat, inv_std


def reference(hidden, norm_gain, emb_table, labels, tok_mask):
    count = jnp.sum(tok_mask)
    vocab_ids = jnp.arange(VOCAB)

    def block_step(carry, block):
        table_grad, gain_grad, loss_sum = carry
        tokens, block_labels, block_mask = block
        normed, x_hat, inv_std = norm_forward(tokens, norm_gain)
        logits = LOGIT_SCALE * jnp.dot(normed, emb_table.T, preferred_element_type=jnp.float32)
        log_norm = jax.nn.logsumexp(logits, axis=-1)
        hits = vocab_ids[None, :] == block_labels[:, None]
        label_logit = jnp.sum(jnp.where(hits, logits, 0.0), axis=-1)
        loss_sum = loss_sum + jnp.sum(block_mask * (log_norm - label_logit))
        soft_probs = jnp.exp(logits - log_norm[:, None])
        weight = block_mask * (LOGIT_SCALE / count)
        d_logits = (jnp.where(hits, soft_probs - 1.0, soft_probs) * weight[:, None]).astype(jnp.bfloat16)
        d_normed = jnp.dot(d_logits, emb_table, preferred_element_type=jnp.float32)
        table_grad = table_grad + jnp.dot(d_logits.T, normed, preferred_element_type=jnp.float32)
        gain_grad = gain_grad + jnp.sum(d_normed * x_hat, axis=0)
        d_xhat = d_normed * norm_gain
        mean_one = jnp.mean(d_xhat, axis=-1, keepdims=True)
        mean_two = jnp.mean(d_xhat * x_hat, axis=-1, keepdims=True)
        d_tokens = inv_std * (d_xhat - mean_one - x_hat * mean_two)
        return (table_grad, gain_grad, loss_sum), d_tokens.astype(jnp.bfloat16)

    blocks = (hidden.reshape(NUM_BLOCKS, BLOCK_TOKENS, WIDTH), labels.reshape(NUM_BLOCKS, BLOCK_TOKENS), tok_mask.reshape(NUM_BLOCKS, BLOCK_TOKENS))
    start = (jnp.zeros((VOCAB, WIDTH), jnp.float32), jnp.zeros((WIDTH,), jnp.float32), jnp.zeros((), jnp.float32))
    (table_grad, gain_grad, loss_sum), d_tokens = lax.scan(block_step, start, blocks)
    return loss_sum / count, table_grad, d_tokens.reshape(BATCH, SEQ_LEN, WIDTH), gain_grad
```

```python
import functools

import jax
import jax.numpy as jnp
from jax import lax
from jax.experimental import pallas as pl
from jax.experimental.pallas import tpu as pltpu
from jax.sharding import PartitionSpec as P

LOGIT_SCALE = 0.0625
EPS = 1e-5
LOG2E = 1.4426950408889634
LN2 = 0.6931471805599453
C2 = LOGIT_SCALE * LOG2E
TB = 256
MIB = 1024 * 1024
NEG = -3e38
MESH = pl.DeviceIdType.MESH


def full(shape):
    return pl.BlockSpec(shape, lambda *_: (0,) * len(shape))


def any_spec():
    return pl.BlockSpec(memory_space=pl.ANY)


def params(limit, **kw):
    return pltpu.CompilerParams(vmem_limit_bytes=limit * MIB, **kw)


def selection(mask_row):
    tokens = mask_row.shape[1]
    rows = lax.broadcasted_iota(jnp.int32, (tokens, tokens), 0)
    cols = lax.broadcasted_iota(jnp.int32, (tokens, tokens), 1)
    upper = jnp.where(rows <= cols, 1.0, 0.0).astype(jnp.bfloat16)
    lhs = jnp.broadcast_to(mask_row, (8, tokens)).astype(jnp.bfloat16)
    rank = jnp.dot(lhs, upper, preferred_element_type=jnp.float32)[0:1]
    hit = (rows.astype(jnp.float32) == rank - 1.0) & (mask_row > 0.0)
    return jnp.where(hit, 1.0, 0.0).astype(jnp.bfloat16)


def normalise(values):
    mean_x = jnp.mean(values, axis=-1, keepdims=True)
    centered = values - mean_x
    variance = jnp.mean(centered * centered, axis=-1, keepdims=True)
    inv_std = lax.rsqrt(variance + EPS)
    return centered * inv_std, inv_std


def prologue(hidden, gain, labels, mask):
    tokens, width = hidden.shape

    def kernel(h_ref, g_ref, l_ref, m_ref, n_ref, nf_ref, hc_ref, meta_ref):
        mask_row = m_ref[...]
        sel = selection(mask_row)
        compact = jnp.dot(sel, h_ref[...], preferred_element_type=jnp.float32)
        hc_ref[...] = compact.astype(jnp.bfloat16)
        x_hat, _ = normalise(compact)
        normed = (g_ref[...] * x_hat).astype(jnp.bfloat16)
        n_ref[...] = normed
        nf_ref[...] = normed.astype(jnp.float32)
        ids = l_ref[...]
        high, mid, low = ids >> 16, (ids >> 8) & 255, ids & 255
        pieces = [p.astype(jnp.float32) for p in (high, mid, low)] + [mask_row]
        stack = jnp.concatenate(pieces + [jnp.zeros((4, tokens), jnp.float32)], axis=0).astype(jnp.bfloat16)
        moved = lax.dot_general(stack, sel, (((1,), (1,)), ((), ())), preferred_element_type=jnp.float32)
        label_row = moved[0:1] * 65536.0 + moved[1:2] * 256.0 + moved[2:3]
        meta_ref[...] = jnp.concatenate([label_row, moved[3:4], jnp.zeros((6, tokens), jnp.float32)], axis=0)

    return pl.pallas_call(
        kernel,
        out_shape=[
            jax.ShapeDtypeStruct((tokens, width), jnp.bfloat16),
            jax.ShapeDtypeStruct((tokens, width), jnp.float32),
            jax.ShapeDtypeStruct((tokens, width), jnp.bfloat16),
            jax.ShapeDtypeStruct((8, tokens), jnp.float32),
        ],
        compiler_params=params(48),
        cost_estimate=pl.CostEstimate(flops=3_000_000_000, bytes_accessed=8_000_000, transcendentals=0),
        name='prologue',
    )(hidden, gain, labels, mask)


def pass_one(count, normed, table, z_in, first_block, total_blocks, tile=2560, slots=6, chunk=256):
    blocks, _, width = normed.shape
    vocab = table.shape[0]
    steps = -(-vocab // tile)
    last = vocab - (steps - 1) * tile
    cast = normed.dtype != jnp.bfloat16

    def kernel(nb_ref, n_ref, e_ref, *rest):
        if z_in is not None:
            rest = rest[1:]
        if cast:
            z_hbm, st_ref, nout_ref, zbuf, sem = rest
        else:
            z_hbm, st_ref, zbuf, sem = rest
            nout_ref = n_ref
        i = pl.program_id(0)
        nb = nb_ref[0]

        @pl.when(i == 0)
        def _():
            st_ref[:, 0:8, :] = jnp.full((blocks, 8, TB), NEG, jnp.float32)
            st_ref[:, 8:16, :] = jnp.zeros((blocks, 8, TB), jnp.float32)
            if cast:
                nout_ref[...] = n_ref[...].astype(jnp.bfloat16)

        def copy(block, slot, rows, base=0):
            return pltpu.make_async_copy(
                zbuf.at[slot, pl.ds(0, rows)], z_hbm.at[first_block + block, pl.ds(base, rows)], sem.at[slot])

        def body(rows):
            def step(j, _):
                g = i * nb + j
                slot = lax.rem(g, slots)

                @pl.when(g >= slots)
                def _():
                    copy(0, slot, tile).wait()

                run_max = st_ref[j, 0:8, :]
                run_sum = st_ref[j, 8:16, :]
                for lo in range(0, rows, chunk):
                    hi = min(lo + chunk, rows)
                    acc = lax.dot_general(e_ref[lo:hi], nout_ref[j], (((1,), (1,)), ((), ())), preferred_element_type=jnp.float32)
                    zbuf[slot, lo:hi, :] = acc
                    parts = acc.reshape((hi - lo) // 8, 8, TB)
                    new_max = jnp.maximum(run_max, jnp.max(parts, axis=0))
                    scaled = new_max * C2
                    total = jnp.sum(jnp.exp2(parts * C2 - scaled[None]), axis=0)
                    run_sum = run_sum * jnp.exp2(run_max * C2 - scaled) + total
                    run_max = new_max
                st_ref[j, 0:8, :] = run_max
                st_ref[j, 8:16, :] = run_sum
                copy(j, slot, rows, i * tile).start()
                return 0

            lax.fori_loop(0, nb, step, 0)

        @pl.when(i < steps - 1)
        def _():
            body(tile)

        @pl.when(i == steps - 1)
        def _():
            body(last)
            end = steps * nb
            for q in range(slots):
                slot = lax.rem(end - 1 - q + slots, slots)

                @pl.when(q < nb)
                def _():
                    copy(0, slot, last).wait()

                @pl.when((q >= nb) & (end - 1 - q >= 0))
                def _():
                    copy(0, slot, tile).wait()

    out_shape = [
        jax.ShapeDtypeStruct((total_blocks, vocab, TB), jnp.float32),
        jax.ShapeDtypeStruct((blocks, 16, TB), jnp.float32),
    ]
    out_specs = [any_spec(), full((blocks, 16, TB))]
    if cast:
        out_shape.append(jax.ShapeDtypeStruct((blocks, TB, width), jnp.bfloat16))
        out_specs.append(full((blocks, TB, width)))
    operands = [count, normed, table]
    in_specs = [full((blocks, TB, width)), pl.BlockSpec((tile, width), lambda i, *_: (i, 0))]
    aliases = {}
    if z_in is not None:
        operands.append(z_in)
        in_specs.append(any_spec())
        aliases = {3: 0}
    return pl.pallas_call(
        kernel,
        grid_spec=pltpu.PrefetchScalarGridSpec(
            num_scalar_prefetch=1, grid=(steps,), in_specs=in_specs, out_specs=out_specs,
            scratch_shapes=[pltpu.VMEM((slots, tile, TB), jnp.float32), pltpu.SemaphoreType.DMA((slots,))]),
        out_shape=out_shape,
        input_output_aliases=aliases,
        compiler_params=params(50),
        cost_estimate=pl.CostEstimate(flops=2 * 2 * TB * vocab * width, bytes_accessed=80_000_000, transcendentals=0),
        name='pass_one',
    )(*operands)


def pass_two(count, order, own, tokf, toki, n_own, n_oth, table, z, tile=1280, slots=6, chunk=256):
    blocks, _, width = n_own.shape
    vocab = table.shape[0]
    steps = -(-vocab // tile)
    last = vocab - (steps - 1) * tile
    halves = tokf.shape[0]

    def kernel(nb_ref, order_ref, own_ref, tf_ref, ti_ref, na_ref, nb2_ref, e_ref, z_hbm, dt_ref, dn_ref, zl_ref,
               n_ref, zbuf, dzbuf, sem):
        i = pl.program_id(0)
        nb = nb_ref[0]
        end = steps * nb

        def copy(g, rows):
            slot = lax.rem(g, slots)
            tile_id = lax.div(g, nb)
            block = order_ref[lax.rem(g, nb)]
            return pltpu.make_async_copy(
                z_hbm.at[block, pl.ds(tile_id * tile, rows)], zbuf.at[slot, pl.ds(0, rows)], sem.at[slot])

        def start(g):
            whole = lax.div(g, nb) < steps - 1

            @pl.when((g < end) & whole)
            def _():
                copy(g, tile).start()

            @pl.when((g < end) & jnp.logical_not(whole))
            def _():
                copy(g, last).start()

        @pl.when(i == 0)
        def _():
            for q in range(slots - 1):
                start(jnp.int32(q))
            dn_ref[...] = jnp.zeros_like(dn_ref)
            zl_ref[...] = jnp.zeros_like(zl_ref)
            n_ref[0:blocks] = na_ref[...]
            n_ref[blocks:] = nb2_ref[...]

        def body(rows):
            def step(j, _):
                block = order_ref[j]
                g = i * nb + j
                slot = lax.rem(g, slots)
                copy(g, rows).wait()
                start(g + slots - 1)
                log_norm = tf_ref[block, 0:1, :]
                weight = tf_ref[block, 1:2, :]
                ids = ti_ref[block, 0:1, :] - i * tile
                picked = jnp.zeros((8, TB), jnp.float32)
                for lo in range(0, rows, chunk):
                    hi = min(lo + chunk, rows)
                    zc = zbuf[slot, lo:hi, :]
                    prob = jnp.exp2(zc * C2 - log_norm)
                    hit = lax.broadcasted_iota(jnp.int32, (hi - lo, TB), 0) == (ids - lo)
                    dz = (jnp.where(hit, prob - 1.0, prob) * weight).astype(jnp.bfloat16)
                    picked = picked + jnp.sum(jnp.where(hit, zc, 0.0).reshape((hi - lo) // 8, 8, TB), axis=0)
                    dzbuf[lo:hi, :] = dz
                zl_ref[block] = zl_ref[block] + picked
                part = jnp.dot(dzbuf[0:rows, :], n_ref[block], preferred_element_type=jnp.float32)
                dt_ref[0:rows, :] = jnp.where(j == 0, 0.0, dt_ref[0:rows, :]) + part
                own_block = own_ref[j]

                @pl.when(own_block >= 0)
                def _():
                    dn_ref[own_block] += lax.dot_general(
                        dzbuf[0:rows, :], e_ref[0:rows, :], (((0,), (0,)), ((), ())), preferred_element_type=jnp.float32)
                return 0

            lax.fori_loop(0, nb, step, 0)

        @pl.when(i < steps - 1)
        def _():
            body(tile)

        @pl.when(i == steps - 1)
        def _():
            body(last)

    return pl.pallas_call(
        kernel,
        grid_spec=pltpu.PrefetchScalarGridSpec(
            num_scalar_prefetch=3, grid=(steps,),
            in_specs=[full((halves, 8, TB)), full((halves, 8, TB)), full((blocks, TB, width)), full((blocks, TB, width)),
                      pl.BlockSpec((tile, width), lambda i, *_: (i, 0)), any_spec()],
            out_specs=[pl.BlockSpec((tile, width), lambda i, *_: (i, 0)), full((blocks, TB, width)), full((halves, 8, TB))],
            scratch_shapes=[pltpu.VMEM((2 * blocks, TB, width), jnp.bfloat16), pltpu.VMEM((slots, tile, TB), jnp.float32),
                            pltpu.VMEM((tile, TB), jnp.bfloat16), pltpu.SemaphoreType.DMA((slots,))]),
        out_shape=[jax.ShapeDtypeStruct((vocab, width), jnp.float32), jax.ShapeDtypeStruct((blocks, TB, width), jnp.float32),
                   jax.ShapeDtypeStruct((halves, 8, TB), jnp.float32)],
        compiler_params=params(56),
        cost_estimate=pl.CostEstimate(flops=6 * 2 * TB * vocab * width, bytes_accessed=200_000_000, transcendentals=0),
        name='pass_two',
    )(count, order, own, tokf, toki, n_own, n_oth, table, z)


def all_to_peers(buf, send_sem, recv_sem, peers):
    me, ids = peers
    copies = []
    for r, (target, _) in enumerate(ids):
        copies.append(pltpu.make_async_remote_copy(
            src_ref=buf.at[me], dst_ref=buf.at[me], send_sem=send_sem.at[r], recv_sem=recv_sem.at[r],
            device_id=target, device_id_type=MESH))
    for c in copies:
        c.start()
    for c in copies:
        c.wait()


def greet(ids):
    barrier = pltpu.get_barrier_semaphore()
    for target, _ in ids:
        pl.semaphore_signal(barrier, inc=1, device_id=target, device_id_type=MESH)
    pl.semaphore_wait(barrier, len(ids))


def combine_stats(st_own, st_oth, mask_own, mask_oth, vp):
    blocks = st_own.shape[0]
    rows = 2 * blocks

    def kernel(a_ref, b_ref, ma_ref, mb_ref, tf_ref, sum_ref, buf, send_sem, recv_sem):
        me = lax.axis_index('vp')
        dp = lax.axis_index('dp')
        ids = [((dp, lax.rem(me + r, vp)), None) for r in range(1, vp)]
        buf[me] = jnp.zeros((16, TB), jnp.float32)
        for k in range(rows):
            st = (a_ref if k < blocks else b_ref)[k % blocks]
            top = jnp.max(st[0:8], axis=0, keepdims=True)
            total = jnp.sum(st[8:16] * jnp.exp2(st[0:8] * C2 - top * C2), axis=0, keepdims=True)
            buf[me, k:k + 1, :] = top
            buf[me, 8 + k:9 + k, :] = total
        greet(ids)
        all_to_peers(buf, send_sem, recv_sem, (me, ids))
        top = buf[0, 0:8, :]
        for k in range(1, vp):
            top = jnp.maximum(top, buf[k, 0:8, :])
        total = jnp.zeros_like(top)
        for k in range(vp):
            total = total + buf[k, 8:16, :] * jnp.exp2((buf[k, 0:8, :] - top) * C2)
        masks = jnp.concatenate([ma_ref[...], mb_ref[...], jnp.zeros((8 - rows, TB), jnp.float32)], axis=0)
        log_norm = top[0:8] * C2 + jnp.log2(total)
        count = jnp.sum(masks)
        weight = masks * (LOGIT_SCALE / count)
        for k in range(rows):
            tf_ref[k] = jnp.concatenate(
                [log_norm[k:k + 1], weight[k:k + 1], jnp.zeros((6, TB), jnp.float32)], axis=0)
        kept = jnp.where(masks > 0.0, log_norm * LN2, 0.0)
        both = jnp.sum(kept[0:blocks]) + jnp.sum(kept[blocks:rows])
        sum_ref[...] = jnp.full((8, 128), both / count, jnp.float32)

    return pl.pallas_call(
        kernel,
        out_shape=[jax.ShapeDtypeStruct((rows, 8, TB), jnp.float32), jax.ShapeDtypeStruct((8, 128), jnp.float32)],
        in_specs=[pl.BlockSpec(memory_space=pltpu.VMEM)] * 4,
        out_specs=[pl.BlockSpec(memory_space=pltpu.VMEM)] * 2,
        scratch_shapes=[pltpu.VMEM((vp, 16, TB), jnp.float32), pltpu.SemaphoreType.DMA((vp - 1,)),
                        pltpu.SemaphoreType.DMA((vp - 1,))],
        compiler_params=pltpu.CompilerParams(collective_id=0, has_side_effects=True),
        name='combine_stats',
    )(st_own, st_oth, mask_own, mask_oth)


def norm_back(d_normed, compact, gain):
    tokens, width = d_normed.shape

    def kernel(dn_ref, h_ref, g_ref, dh_ref, dg_ref):
        dn = dn_ref[...]
        x_hat, inv_std = normalise(h_ref[...].astype(jnp.float32))
        scaled = dn * g_ref[...]
        mean_one = jnp.mean(scaled, axis=-1, keepdims=True)
        mean_two = jnp.mean(scaled * x_hat, axis=-1, keepdims=True)
        grad = (inv_std * (scaled - mean_one - x_hat * mean_two)).astype(jnp.bfloat16)
        dh_ref[...] = grad.astype(jnp.float32)
        dg_ref[...] = jnp.sum((dn * x_hat).reshape(tokens // 8, 8, width), axis=0)

    return pl.pallas_call(
        kernel,
        out_shape=[jax.ShapeDtypeStruct((tokens, width), jnp.float32), jax.ShapeDtypeStruct((8, width), jnp.float32)],
        name='norm_back',
    )(d_normed, compact, gain)


def total_gain(partial, picked, masks, dp_size, vp):
    width = partial.shape[1]
    group = dp_size * vp

    def kernel(p_ref, z_ref, m_ref, dg_ref, zl_ref, buf, send_sem, recv_sem):
        my_dp = lax.axis_index('dp')
        my_vp = lax.axis_index('vp')
        me = my_dp * vp + my_vp
        ids = []
        for r in range(1, group):
            other = lax.rem(me + r, group)
            ids.append(((lax.div(other, vp), lax.rem(other, vp)), None))
        buf[me, 0:1, :] = jnp.sum(p_ref[...], axis=0, keepdims=True)
        masks = m_ref[...]
        kept = jnp.where(masks > 0.0, jnp.sum(z_ref[...], axis=1), 0.0)
        half = kept.shape[0] // 2
        both = jnp.sum(kept[:half]) + jnp.sum(kept[half:])
        buf[me, 1:2, :] = jnp.full((1, width), both * LOGIT_SCALE / jnp.sum(masks), jnp.float32)
        buf[me, 2:8, :] = jnp.zeros((6, width), jnp.float32)
        greet(ids)
        all_to_peers(buf, send_sem, recv_sem, (me, ids))
        total = buf[0]
        for k in range(1, group):
            total = total + buf[k]
        dg_ref[...] = total[0:1]
        zl_ref[...] = total[1:2] * (1.0 / dp_size)

    return pl.pallas_call(
        kernel,
        out_shape=[jax.ShapeDtypeStruct((1, width), jnp.float32), jax.ShapeDtypeStruct((1, width), jnp.float32)],
        in_specs=[pl.BlockSpec(memory_space=pltpu.VMEM)] * 3,
        out_specs=[pl.BlockSpec(memory_space=pltpu.VMEM)] * 2,
        scratch_shapes=[pltpu.VMEM((group, 8, width), jnp.float32), pltpu.SemaphoreType.DMA((group - 1,)),
                        pltpu.SemaphoreType.DMA((group - 1,))],
        compiler_params=pltpu.CompilerParams(collective_id=1, has_side_effects=True),
        name='total_gain',
    )(partial, picked, masks)


def scatter_tokens(grads, mask):
    tokens, width = grads.shape

    def kernel(g_ref, m_ref, o_ref):
        sel = selection(m_ref[...])
        o_ref[...] = lax.dot_general(
            sel, g_ref[...].astype(jnp.bfloat16), (((0,), (0,)), ((), ())), preferred_element_type=jnp.float32).astype(jnp.bfloat16)

    return pl.pallas_call(
        kernel, out_shape=jax.ShapeDtypeStruct((tokens, width), jnp.bfloat16), compiler_params=params(48), name='scatter_tokens',
    )(grads, mask)


def solution(mesh):
    dp_size, vp = mesh.shape['dp'], mesh.shape['vp']

    def local_step(hidden, norm_gain, emb_table, labels, tok_mask):
        rows, seq_len, width = hidden.shape
        vocab = emb_table.shape[0]
        tokens = rows * seq_len
        blocks = tokens // TB
        share = tokens // vp
        my_vp = lax.axis_index('vp')
        my_dp = lax.axis_index('dp')
        gain = norm_gain.reshape(1, width)
        mask_row = tok_mask.reshape(1, tokens)
        n_own, n_wide, compact, meta = prologue(hidden.reshape(tokens, width), gain, labels.reshape(1, tokens), mask_row)
        swap = [(0, 1), (1, 0)]
        meta_oth = lax.ppermute(meta, 'dp', swap)
        piece = lax.ppermute(lax.dynamic_slice_in_dim(n_wide, my_vp * share, share, 0), 'dp', swap)
        n_oth_wide = lax.all_gather(piece, 'vp', axis=0, tiled=True).reshape(blocks, TB, width)
        n_own = n_own.reshape(blocks, TB, width)

        def block_count(m):
            return lax.div(jnp.sum(m[1]).astype(jnp.int32) + (TB - 1), TB)

        nb_own, nb_oth = block_count(meta), block_count(meta_oth)
        z, st_own = pass_one(nb_own[None], n_own, emb_table, None, 0, 2 * blocks)
        z, st_oth, n_oth = pass_one(nb_oth[None], n_oth_wide, emb_table, z, blocks, 2 * blocks)
        mask_own, mask_oth = meta[1].reshape(blocks, TB), meta_oth[1].reshape(blocks, TB)
        tokf, lse_sum = combine_stats(st_own, st_oth, mask_own, mask_oth, vp)
        ids = jnp.concatenate([meta[0], meta_oth[0]]).astype(jnp.int32).reshape(2 * blocks, 1, TB) - my_vp * vocab
        toki = jnp.broadcast_to(ids, (2 * blocks, 8, TB))
        j = jnp.arange(2 * blocks, dtype=jnp.int32)
        first = jnp.where(my_dp == 0, nb_own, nb_oth)
        in_first = j < first
        is_own = in_first == (my_dp == 0)
        local = jnp.where(in_first, j, j - first)
        order = jnp.clip(jnp.where(is_own, local, local + blocks), 0, 2 * blocks - 1)
        own = jnp.where(is_own, jnp.minimum(local, blocks - 1), -1)
        d_table, d_part, picked = pass_two(
            (nb_own + nb_oth)[None], order, own, tokf, toki, n_own, n_oth, emb_table, z)
        d_share = lax.psum_scatter(d_part.reshape(tokens, width), 'vp', scatter_dimension=0, tiled=True)
        mine = lax.dynamic_slice_in_dim(compact, my_vp * share, share, 0)
        grads, gain_part = norm_back(d_share, mine, gain)
        all_grads = lax.all_gather(grads, 'vp', axis=0, tiled=True)
        d_gain, label_sum = total_gain(gain_part, picked, jnp.concatenate([mask_own, mask_oth]), dp_size, vp)
        d_hidden = scatter_tokens(all_grads, mask_row)
        loss = lse_sum[0, 0] - label_sum[0, 0]
        return loss, d_table, d_hidden.reshape(rows, seq_len, width), d_gain.reshape(width)

    return jax.shard_map(
        local_step, mesh=mesh,
        in_specs=(P('dp', None, None), P(None), P('vp', None), P('dp', None), P('dp', None)),
        out_specs=(P(), P('vp', None), P('dp', None, None), P(None)), check_vma=False)
```

```python
import functools

import jax
import jax.numpy as jnp
from jax import lax
from jax.experimental import pallas as pl
from jax.experimental.pallas import tpu as pltpu
from jax.sharding import PartitionSpec as P

LOGIT_SCALE = 0.0625
EPS = 1e-5
LOG2E = 1.4426950408889634
LN2 = 0.6931471805599453
C2 = LOGIT_SCALE * LOG2E
TB = 256
SPLIT = 9
MIB = 1024 * 1024
NEG = -3e38
MESH = pl.DeviceIdType.MESH


def full(shape):
    return pl.BlockSpec(shape, lambda *_: (0,) * len(shape))


def any_spec():
    return pl.BlockSpec(memory_space=pl.ANY)


def params(limit, **kw):
    return pltpu.CompilerParams(vmem_limit_bytes=limit * MIB, **kw)


def selection(mask_row):
    tokens = mask_row.shape[1]
    rows = lax.broadcasted_iota(jnp.int32, (tokens, tokens), 0)
    cols = lax.broadcasted_iota(jnp.int32, (tokens, tokens), 1)
    upper = jnp.where(rows <= cols, 1.0, 0.0).astype(jnp.bfloat16)
    lhs = jnp.broadcast_to(mask_row, (8, tokens)).astype(jnp.bfloat16)
    rank = jnp.dot(lhs, upper, preferred_element_type=jnp.float32)[0:1]
    hit = (rows.astype(jnp.float32) == rank - 1.0) & (mask_row > 0.0)
    return jnp.where(hit, 1.0, 0.0).astype(jnp.bfloat16)


def normalise(values):
    mean_x = jnp.mean(values, axis=-1, keepdims=True)
    centered = values - mean_x
    variance = jnp.mean(centered * centered, axis=-1, keepdims=True)
    inv_std = lax.rsqrt(variance + EPS)
    return centered * inv_std, inv_std


def prologue(hidden, gain, labels, mask):
    tokens, width = hidden.shape

    def kernel(h_ref, g_ref, l_ref, m_ref, n_ref, nf_ref, hc_ref, meta_ref):
        mask_row = m_ref[...]
        sel = selection(mask_row)
        compact = jnp.dot(sel, h_ref[...], preferred_element_type=jnp.float32)
        hc_ref[...] = compact.astype(jnp.bfloat16)
        x_hat, _ = normalise(compact)
        normed = (g_ref[...] * x_hat).astype(jnp.bfloat16)
        n_ref[...] = normed
        nf_ref[...] = normed.astype(jnp.float32)
        ids = l_ref[...]
        high, mid, low = ids >> 16, (ids >> 8) & 255, ids & 255
        pieces = [p.astype(jnp.float32) for p in (high, mid, low)] + [mask_row]
        stack = jnp.concatenate(pieces + [jnp.zeros((4, tokens), jnp.float32)], axis=0).astype(jnp.bfloat16)
        moved = lax.dot_general(stack, sel, (((1,), (1,)), ((), ())), preferred_element_type=jnp.float32)
        label_row = moved[0:1] * 65536.0 + moved[1:2] * 256.0 + moved[2:3]
        meta_ref[...] = jnp.concatenate([label_row, moved[3:4], jnp.zeros((6, tokens), jnp.float32)], axis=0)

    return pl.pallas_call(
        kernel,
        out_shape=[
            jax.ShapeDtypeStruct((tokens, width), jnp.bfloat16),
            jax.ShapeDtypeStruct((tokens, width), jnp.float32),
            jax.ShapeDtypeStruct((tokens, width), jnp.bfloat16),
            jax.ShapeDtypeStruct((8, tokens), jnp.float32),
        ],
        compiler_params=params(48),
        cost_estimate=pl.CostEstimate(flops=3_000_000_000, bytes_accessed=8_000_000, transcendentals=0),
        name='prologue',
    )(hidden, gain, labels, mask)


def pass_one(count, normed, table, z_in, first_block, total_blocks, tile=2560, slots=6, chunk=256):
    blocks, _, width = normed.shape
    vocab = table.shape[0]
    steps = -(-vocab // tile)
    last = vocab - (steps - 1) * tile
    cast = normed.dtype != jnp.bfloat16

    def kernel(nb_ref, n_ref, e_ref, *rest):
        if z_in is not None:
            rest = rest[1:]
        if cast:
            z_hbm, st_ref, nout_ref, zbuf, sem = rest
        else:
            z_hbm, st_ref, zbuf, sem = rest
            nout_ref = n_ref
        i = pl.program_id(0)
        nb = nb_ref[0]

        @pl.when(i == 0)
        def _():
            st_ref[:, 0:8, :] = jnp.full((blocks, 8, TB), NEG, jnp.float32)
            st_ref[:, 8:16, :] = jnp.zeros((blocks, 8, TB), jnp.float32)
            if cast:
                nout_ref[...] = n_ref[...].astype(jnp.bfloat16)

        def copy(block, slot, rows, base=0):
            return pltpu.make_async_copy(
                zbuf.at[slot, pl.ds(0, rows)], z_hbm.at[first_block + block, pl.ds(base, rows)], sem.at[slot])

        def body(rows):
            def step(j, _):
                g = i * nb + j
                slot = lax.rem(g, slots)

                @pl.when(g >= slots)
                def _():
                    copy(0, slot, tile).wait()

                run_max = st_ref[j, 0:8, :]
                run_sum = st_ref[j, 8:16, :]
                for lo in range(0, rows, chunk):
                    hi = min(lo + chunk, rows)
                    acc = C2 * lax.dot_general(
                        e_ref[lo:hi], nout_ref[j], (((1,), (1,)), ((), ())), preferred_element_type=jnp.float32)
                    zbuf[slot, lo:hi, :] = acc
                    parts = acc.reshape((hi - lo) // 8, 8, TB)
                    new_max = jnp.maximum(run_max, jnp.max(parts, axis=0))
                    total = jnp.sum(jnp.exp2(parts - new_max[None]), axis=0)
                    run_sum = run_sum * jnp.exp2(run_max - new_max) + total
                    run_max = new_max
                st_ref[j, 0:8, :] = run_max
                st_ref[j, 8:16, :] = run_sum
                copy(j, slot, rows, i * tile).start()
                return 0

            lax.fori_loop(0, nb, step, 0)

        @pl.when(i < steps - 1)
        def _():
            body(tile)

        @pl.when(i == steps - 1)
        def _():
            body(last)
            end = steps * nb
            for q in range(slots):
                slot = lax.rem(end - 1 - q + slots, slots)

                @pl.when(q < nb)
                def _():
                    copy(0, slot, last).wait()

                @pl.when((q >= nb) & (end - 1 - q >= 0))
                def _():
                    copy(0, slot, tile).wait()

    out_shape = [
        jax.ShapeDtypeStruct((total_blocks, vocab, TB), jnp.float32),
        jax.ShapeDtypeStruct((blocks, 16, TB), jnp.float32),
    ]
    out_specs = [any_spec(), full((blocks, 16, TB))]
    if cast:
        out_shape.append(jax.ShapeDtypeStruct((blocks, TB, width), jnp.bfloat16))
        out_specs.append(full((blocks, TB, width)))
    operands = [count, normed, table]
    in_specs = [full((blocks, TB, width)), pl.BlockSpec((tile, width), lambda i, *_: (i, 0))]
    aliases = {}
    if z_in is not None:
        operands.append(z_in)
        in_specs.append(any_spec())
        aliases = {3: 0}
    return pl.pallas_call(
        kernel,
        grid_spec=pltpu.PrefetchScalarGridSpec(
            num_scalar_prefetch=1, grid=(steps,), in_specs=in_specs, out_specs=out_specs,
            scratch_shapes=[pltpu.VMEM((slots, tile, TB), jnp.float32), pltpu.SemaphoreType.DMA((slots,))]),
        out_shape=out_shape,
        input_output_aliases=aliases,
        compiler_params=params(50),
        cost_estimate=pl.CostEstimate(flops=2 * 2 * TB * vocab * width, bytes_accessed=80_000_000, transcendentals=0),
        name='pass_one',
    )(*operands)


def d_logits(zc, lo, shift, weight, ids):
    scaled = jnp.exp2(zc - shift)
    hit = lax.broadcasted_iota(jnp.int32, zc.shape, 0) == (ids - lo)
    dz = jnp.where(hit, scaled - weight, scaled).astype(jnp.bfloat16)
    picked = jnp.where(hit, zc, 0.0)
    return dz, jnp.sum(picked.reshape(zc.shape[0] // 8, 8, zc.shape[1]), axis=0)


def loop(count, f):
    lax.fori_loop(0, count, lambda j, _: (f(j), 0)[1], 0)


def pass_two_own(count, tokf, toki, table, z, blocks, tile=1280, chunk=256):
    vocab, width = table.shape
    steps = -(-vocab // tile)
    last = vocab - (steps - 1) * tile

    def kernel(nb_ref, tf_ref, ti_ref, e_ref, z_hbm, dz_hbm, dn_ref, zl_ref, za, zb, da, db, zsem, dsem):
        i = pl.program_id(0)
        nb = nb_ref[0]
        zs, ds = (za, zb), (da, db)

        def zcopy(par, j, t, rows):
            return pltpu.make_async_copy(
                z_hbm.at[j, pl.ds(t * tile, rows)], zs[par].at[j, pl.ds(0, rows)], zsem.at[par, j])

        def dcopy(par, j, t, rows):
            return pltpu.make_async_copy(
                ds[par].at[j, pl.ds(0, rows)], dz_hbm.at[j, pl.ds(t * tile, rows)], dsem.at[par, j])

        def make(par, t, j, rows):
            ids = ti_ref[j, 0:1, :] - t * tile
            total = jnp.zeros((8, TB), jnp.float32)
            for lo in range(0, rows, chunk):
                hi = min(lo + chunk, rows)
                dz, picked = d_logits(zs[par][j, lo:hi, :], lo, tf_ref[j, 0:1, :], tf_ref[j, 1:2, :], ids)
                ds[par][j, lo:hi, :] = dz
                total = total + picked
            zl_ref[j] = zl_ref[j] + total

        def product(par, j, rows):
            dn_ref[j] += lax.dot_general(
                ds[par][j, 0:rows, :], e_ref[0:rows, :], (((0,), (0,)), ((), ())), preferred_element_type=jnp.float32)

        @pl.when(i == 0)
        def _():
            dn_ref[...] = jnp.zeros_like(dn_ref)
            zl_ref[...] = jnp.zeros_like(zl_ref)
            loop(nb, lambda j: zcopy(0, j, 0, tile).start())
            loop(nb, lambda j: zcopy(1, j, 1, tile).start())

            def first(j):
                zcopy(0, j, 0, tile).wait()
                make(0, 0, j, tile)
                dcopy(0, j, 0, tile).start()

            loop(nb, first)

        def variant(par, next_rows):
            @pl.when(i + 2 < steps - 1)
            def _():
                loop(nb, lambda j: zcopy(par, j, i + 2, tile).start())

            @pl.when(i + 2 == steps - 1)
            def _():
                loop(nb, lambda j: zcopy(par, j, i + 2, last).start())

            def f(j):
                zcopy(1 - par, j, 0, next_rows).wait()

                @pl.when(i >= 1)
                def _():
                    dcopy(1 - par, j, 0, tile).wait()

                product(par, j, tile)
                make(1 - par, i + 1, j, next_rows)
                dcopy(1 - par, j, i + 1, next_rows).start()

            loop(nb, f)

        end = (steps - 1) % 2
        for par in (0, 1):
            @pl.when((i < steps - 2) & (lax.rem(i, 2) == par))
            def _():
                variant(par, tile)

        @pl.when(i == steps - 2)
        def _():
            variant(1 - end, last)

        @pl.when(i == steps - 1)
        def _():
            def f(j):
                product(end, j, last)
                dcopy(end, j, 0, last).wait()
                dcopy(1 - end, j, 0, tile).wait()

            loop(nb, f)

    halves = tokf.shape[0]
    return pl.pallas_call(
        kernel,
        grid_spec=pltpu.PrefetchScalarGridSpec(
            num_scalar_prefetch=1, grid=(steps,),
            in_specs=[full((halves, 8, TB)), full((halves, 8, TB)), pl.BlockSpec((tile, width), lambda i, *_: (i, 0)),
                      any_spec()],
            out_specs=[any_spec(), full((blocks, TB, width)), full((blocks, 8, TB))],
            scratch_shapes=[pltpu.VMEM((blocks, tile, TB), jnp.float32)] * 2
            + [pltpu.VMEM((blocks, tile, TB), jnp.bfloat16)] * 2 + [pltpu.SemaphoreType.DMA((2, blocks))] * 2),
        out_shape=[jax.ShapeDtypeStruct((blocks, vocab, TB), jnp.bfloat16),
                   jax.ShapeDtypeStruct((blocks, TB, width), jnp.float32), jax.ShapeDtypeStruct((blocks, 8, TB), jnp.float32)],
        compiler_params=params(56),
        cost_estimate=pl.CostEstimate(flops=4 * TB * vocab * width, bytes_accessed=100_000_000, transcendentals=0),
        name='pass_two_own',
    )(count, tokf, toki, table, z)


def pass_two_table(counts, order, tokf, toki, n_own, n_oth, dz_own, z, d_table, after, t0, t1, tile=1280, chunk=256):
    blocks, _, width = n_own.shape
    vocab = z.shape[1]
    steps = -(-vocab // tile)
    last = vocab - (steps - 1) * tile
    halves = 2 * blocks

    def kernel(sc_ref, order_ref, tf_ref, ti_ref, na_ref, nb_ref, dz_hbm, z_hbm, *rest):
        if d_table is not None:
            rest = rest[2:]
        dt_ref, zl_ref, n_ref, za, zb, da, db, zsem, dsem = rest
        i = pl.program_id(0)
        t = i + t0
        own, oth = sc_ref[0], sc_ref[1]
        zs, ds = (za, zb), (da, db)

        def zcopy(par, j, tile_id, rows):
            return pltpu.make_async_copy(
                z_hbm.at[blocks + j, pl.ds(tile_id * tile, rows)], zs[par].at[j, pl.ds(0, rows)], zsem.at[par, j])

        def dcopy(par, j, tile_id, rows):
            return pltpu.make_async_copy(
                dz_hbm.at[j, pl.ds(tile_id * tile, rows)], ds[par].at[j, pl.ds(0, rows)], dsem.at[par, j])

        def load(copy, count, par, tile_id):
            @pl.when((tile_id < t1) & (tile_id < steps - 1))
            def _():
                loop(count, lambda j: copy(par, j, tile_id, tile).start())

            @pl.when((tile_id < t1) & (tile_id == steps - 1))
            def _():
                loop(count, lambda j: copy(par, j, tile_id, last).start())

        def arrive(copy, count, par, tile_id):
            @pl.when((tile_id < t1) & (tile_id < steps - 1))
            def _():
                loop(count, lambda j: copy(par, j, 0, tile).wait())

            @pl.when((tile_id < t1) & (tile_id == steps - 1))
            def _():
                loop(count, lambda j: copy(par, j, 0, last).wait())

        def make(par, tile_id, j):
            ids = ti_ref[blocks + j, 0:1, :] - tile_id * tile
            total = jnp.zeros((8, TB), jnp.float32)
            for lo in range(0, tile, chunk):
                hi = min(lo + chunk, tile)
                dz, picked = d_logits(
                    zs[par][j, lo:hi, :], lo, tf_ref[blocks + j, 0:1, :], tf_ref[blocks + j, 1:2, :], ids)
                ds[par][blocks + j, lo:hi, :] = dz
                total = total + picked
            zl_ref[j] = zl_ref[j] + jnp.where(tile_id < t1, total, 0.0)

        def product(par, j, first):
            block = order_ref[j]
            part = jnp.dot(ds[par][block], n_ref[block], preferred_element_type=jnp.float32)
            if first:
                dt_ref[...] = part
            else:
                dt_ref[...] += part

        @pl.when(i == 0)
        def _():
            zl_ref[...] = jnp.zeros_like(zl_ref)
            load(zcopy, oth, 0, t0)
            load(dcopy, own, 0, t0)
            load(zcopy, oth, 1, t0 + 1)
            n_ref[0:blocks] = na_ref[...]
            n_ref[blocks:] = nb_ref[...]
            arrive(zcopy, oth, 0, t0)
            loop(oth, lambda j: make(0, t0, j))

        def variant(par):
            arrive(dcopy, own, par, t)
            arrive(zcopy, oth, 1 - par, t + 1)
            load(zcopy, oth, par, t + 2)
            load(dcopy, own, 1 - par, t + 1)
            product(par, 0, True)
            make(1 - par, t + 1, 0)

            def both(j, _):
                product(par, j, False)
                make(1 - par, t + 1, j)
                return 0

            def single(j, _):
                product(par, j, False)
                return 0

            lax.fori_loop(1, oth, both, 0)
            lax.fori_loop(oth, own + oth, single, 0)

        for par in (0, 1):
            @pl.when(lax.rem(i, 2) == par)
            def _():
                variant(par)

    operands = [counts, order, tokf, toki, n_own, n_oth, dz_own, z]
    in_specs = [full((halves, 8, TB)), full((halves, 8, TB)), full((blocks, TB, width)), full((blocks, TB, width)),
                any_spec(), any_spec()]
    aliases = {}
    if d_table is not None:
        operands += [d_table, after]
        in_specs += [any_spec(), any_spec()]
        aliases = {8: 0}
    return pl.pallas_call(
        kernel,
        grid_spec=pltpu.PrefetchScalarGridSpec(
            num_scalar_prefetch=2, grid=(t1 - t0,), in_specs=in_specs,
            out_specs=[pl.BlockSpec((tile, width), lambda i, *_: (i + t0, 0)), full((blocks, 8, TB))],
            scratch_shapes=[pltpu.VMEM((halves, TB, width), jnp.bfloat16)]
            + [pltpu.VMEM((blocks, tile, TB), jnp.float32)] * 2 + [pltpu.VMEM((halves, tile, TB), jnp.bfloat16)] * 2
            + [pltpu.SemaphoreType.DMA((2, blocks))] * 2),
        out_shape=[jax.ShapeDtypeStruct((vocab, width), jnp.float32), jax.ShapeDtypeStruct((blocks, 8, TB), jnp.float32)],
        input_output_aliases=aliases,
        compiler_params=params(52),
        cost_estimate=pl.CostEstimate(
            flops=8 * TB * vocab * width * (t1 - t0) // steps, bytes_accessed=100_000_000, transcendentals=0),
        name='pass_two_table',
    )(*operands)


def all_to_peers(buf, send_sem, recv_sem, peers):
    me, ids = peers
    copies = []
    for r, (target, _) in enumerate(ids):
        copies.append(pltpu.make_async_remote_copy(
            src_ref=buf.at[me], dst_ref=buf.at[me], send_sem=send_sem.at[r], recv_sem=recv_sem.at[r],
            device_id=target, device_id_type=MESH))
    for c in copies:
        c.start()
    for c in copies:
        c.wait()


def greet(ids):
    barrier = pltpu.get_barrier_semaphore()
    for target, _ in ids:
        pl.semaphore_signal(barrier, inc=1, device_id=target, device_id_type=MESH)
    pl.semaphore_wait(barrier, len(ids))


def combine_stats(st_own, st_oth, mask_own, mask_oth, vp):
    blocks = st_own.shape[0]
    rows = 2 * blocks

    def kernel(a_ref, b_ref, ma_ref, mb_ref, tf_ref, sum_ref, buf, send_sem, recv_sem):
        me = lax.axis_index('vp')
        dp = lax.axis_index('dp')
        ids = [((dp, lax.rem(me + r, vp)), None) for r in range(1, vp)]
        buf[me] = jnp.zeros((16, TB), jnp.float32)
        for k in range(rows):
            st = (a_ref if k < blocks else b_ref)[k % blocks]
            top = jnp.max(st[0:8], axis=0, keepdims=True)
            total = jnp.sum(st[8:16] * jnp.exp2(st[0:8] - top), axis=0, keepdims=True)
            buf[me, k:k + 1, :] = top
            buf[me, 8 + k:9 + k, :] = total
        greet(ids)
        all_to_peers(buf, send_sem, recv_sem, (me, ids))
        top = buf[0, 0:8, :]
        for k in range(1, vp):
            top = jnp.maximum(top, buf[k, 0:8, :])
        total = jnp.zeros_like(top)
        for k in range(vp):
            total = total + buf[k, 8:16, :] * jnp.exp2(buf[k, 0:8, :] - top)
        masks = jnp.concatenate([ma_ref[...], mb_ref[...], jnp.zeros((8 - rows, TB), jnp.float32)], axis=0)
        log_norm = top + jnp.log2(total)
        count = jnp.sum(masks)
        weight = masks * (LOGIT_SCALE / count)
        shift = log_norm - jnp.log2(weight)
        for k in range(rows):
            tf_ref[k] = jnp.concatenate(
                [shift[k:k + 1], weight[k:k + 1], jnp.zeros((6, TB), jnp.float32)], axis=0)
        kept = jnp.where(masks > 0.0, log_norm * LN2, 0.0)
        both = jnp.sum(kept[0:blocks]) + jnp.sum(kept[blocks:rows])
        sum_ref[...] = jnp.full((8, 128), both / count, jnp.float32)

    return pl.pallas_call(
        kernel,
        out_shape=[jax.ShapeDtypeStruct((rows, 8, TB), jnp.float32), jax.ShapeDtypeStruct((8, 128), jnp.float32)],
        in_specs=[pl.BlockSpec(memory_space=pltpu.VMEM)] * 4,
        out_specs=[pl.BlockSpec(memory_space=pltpu.VMEM)] * 2,
        scratch_shapes=[pltpu.VMEM((vp, 16, TB), jnp.float32), pltpu.SemaphoreType.DMA((vp - 1,)),
                        pltpu.SemaphoreType.DMA((vp - 1,))],
        compiler_params=pltpu.CompilerParams(collective_id=0, has_side_effects=True),
        name='combine_stats',
    )(st_own, st_oth, mask_own, mask_oth)


def norm_back(d_normed, compact, gain, after):
    tokens, width = d_normed.shape

    def kernel(dn_ref, h_ref, g_ref, _, dh_ref, dg_ref):
        dn = dn_ref[...]
        x_hat, inv_std = normalise(h_ref[...].astype(jnp.float32))
        scaled = dn * g_ref[...]
        mean_one = jnp.mean(scaled, axis=-1, keepdims=True)
        mean_two = jnp.mean(scaled * x_hat, axis=-1, keepdims=True)
        grad = (inv_std * (scaled - mean_one - x_hat * mean_two)).astype(jnp.bfloat16)
        dh_ref[...] = grad.astype(jnp.float32)
        dg_ref[...] = jnp.sum((dn * x_hat).reshape(tokens // 8, 8, width), axis=0)

    return pl.pallas_call(
        kernel,
        out_shape=[jax.ShapeDtypeStruct((tokens, width), jnp.float32), jax.ShapeDtypeStruct((8, width), jnp.float32)],
        in_specs=[pl.BlockSpec(memory_space=pltpu.VMEM)] * 3 + [any_spec()],
        name='norm_back',
    )(d_normed, compact, gain, after)


def total_gain(partial, picked, masks, dp_size, vp):
    width = partial.shape[1]
    group = dp_size * vp

    def kernel(p_ref, z_ref, m_ref, dg_ref, zl_ref, buf, send_sem, recv_sem):
        my_dp = lax.axis_index('dp')
        my_vp = lax.axis_index('vp')
        me = my_dp * vp + my_vp
        ids = []
        for r in range(1, group):
            other = lax.rem(me + r, group)
            ids.append(((lax.div(other, vp), lax.rem(other, vp)), None))
        buf[me, 0:1, :] = jnp.sum(p_ref[...], axis=0, keepdims=True)
        masks = m_ref[...]
        kept = jnp.where(masks > 0.0, jnp.sum(z_ref[...], axis=1), 0.0)
        half = kept.shape[0] // 2
        both = jnp.sum(kept[:half]) + jnp.sum(kept[half:])
        buf[me, 1:2, :] = jnp.full((1, width), both * LN2 / jnp.sum(masks), jnp.float32)
        buf[me, 2:8, :] = jnp.zeros((6, width), jnp.float32)
        greet(ids)
        all_to_peers(buf, send_sem, recv_sem, (me, ids))
        total = buf[0]
        for k in range(1, group):
            total = total + buf[k]
        dg_ref[...] = total[0:1]
        zl_ref[...] = total[1:2] * (1.0 / dp_size)

    return pl.pallas_call(
        kernel,
        out_shape=[jax.ShapeDtypeStruct((1, width), jnp.float32), jax.ShapeDtypeStruct((1, width), jnp.float32)],
        in_specs=[pl.BlockSpec(memory_space=pltpu.VMEM)] * 3,
        out_specs=[pl.BlockSpec(memory_space=pltpu.VMEM)] * 2,
        scratch_shapes=[pltpu.VMEM((group, 8, width), jnp.float32), pltpu.SemaphoreType.DMA((group - 1,)),
                        pltpu.SemaphoreType.DMA((group - 1,))],
        compiler_params=pltpu.CompilerParams(collective_id=1, has_side_effects=True),
        name='total_gain',
    )(partial, picked, masks)


def scatter_tokens(grads, mask):
    tokens, width = grads.shape

    def kernel(g_ref, m_ref, o_ref):
        sel = selection(m_ref[...])
        o_ref[...] = lax.dot_general(
            sel, g_ref[...].astype(jnp.bfloat16), (((0,), (0,)), ((), ())), preferred_element_type=jnp.float32).astype(jnp.bfloat16)

    return pl.pallas_call(
        kernel, out_shape=jax.ShapeDtypeStruct((tokens, width), jnp.bfloat16), compiler_params=params(48), name='scatter_tokens',
    )(grads, mask)


def solution(mesh):
    dp_size, vp = mesh.shape['dp'], mesh.shape['vp']

    def local_step(hidden, norm_gain, emb_table, labels, tok_mask):
        rows, seq_len, width = hidden.shape
        vocab = emb_table.shape[0]
        tokens = rows * seq_len
        blocks = tokens // TB
        share = tokens // vp
        my_vp = lax.axis_index('vp')
        my_dp = lax.axis_index('dp')
        gain = norm_gain.reshape(1, width)
        mask_row = tok_mask.reshape(1, tokens)
        n_own, n_wide, compact, meta = prologue(hidden.reshape(tokens, width), gain, labels.reshape(1, tokens), mask_row)
        swap = [(0, 1), (1, 0)]
        meta_oth = lax.ppermute(meta, 'dp', swap)
        piece = lax.ppermute(lax.dynamic_slice_in_dim(n_wide, my_vp * share, share, 0), 'dp', swap)
        n_oth_wide = lax.all_gather(piece, 'vp', axis=0, tiled=True).reshape(blocks, TB, width)
        n_own = n_own.reshape(blocks, TB, width)

        def block_count(m):
            return lax.div(jnp.sum(m[1]).astype(jnp.int32) + (TB - 1), TB)

        nb_own, nb_oth = block_count(meta), block_count(meta_oth)
        z, st_own = pass_one(nb_own[None], n_own, emb_table, None, 0, 2 * blocks)
        z, st_oth, n_oth = pass_one(nb_oth[None], n_oth_wide, emb_table, z, blocks, 2 * blocks)
        mask_own, mask_oth = meta[1].reshape(blocks, TB), meta_oth[1].reshape(blocks, TB)
        tokf, lse_sum = combine_stats(st_own, st_oth, mask_own, mask_oth, vp)
        ids = jnp.concatenate([meta[0], meta_oth[0]]).astype(jnp.int32).reshape(2 * blocks, 1, TB) - my_vp * vocab
        ids = jnp.where((ids >= 0) & (ids < vocab), ids, -vocab)
        toki = jnp.broadcast_to(ids, (2 * blocks, 8, TB))
        j = jnp.arange(2 * blocks, dtype=jnp.int32)
        first = jnp.where(my_dp == 0, nb_own, nb_oth)
        in_first = j < first
        is_own = in_first == (my_dp == 0)
        local = jnp.where(in_first, j, j - first)
        order = jnp.clip(jnp.where(is_own, local, local + blocks), 0, 2 * blocks - 1)
        counts = jnp.stack([nb_own, nb_oth])
        dz_own, d_part, picked = pass_two_own(nb_own[None], tokf, toki, emb_table, z, blocks)
        d_share = lax.psum_scatter(d_part.reshape(tokens, width), 'vp', scatter_dimension=0, tiled=True)
        args = (counts, order, tokf, toki, n_own, n_oth, dz_own, z)
        steps, cut = -(-vocab // 1280), SPLIT
        d_table, picked_a = pass_two_table(*args, None, None, 0, cut)
        mine = lax.dynamic_slice_in_dim(compact, my_vp * share, share, 0)
        grads, gain_part = norm_back(d_share, mine, gain, picked_a)
        d_table, picked_b = pass_two_table(*args, d_table, gain_part, cut, steps)
        all_grads = lax.all_gather(grads, 'vp', axis=0, tiled=True)
        d_gain, label_sum = total_gain(gain_part, jnp.concatenate([picked, picked_a + picked_b]), jnp.concatenate([mask_own, mask_oth]), dp_size, vp)
        d_hidden = scatter_tokens(all_grads, mask_row)
        loss = lse_sum[0, 0] - label_sum[0, 0]
        return loss, d_table, d_hidden.reshape(rows, seq_len, width), d_gain.reshape(width)

    return jax.shard_map(
        local_step, mesh=mesh,
        in_specs=(P('dp', None, None), P(None), P('vp', None), P('dp', None), P('dp', None)),
        out_specs=(P(), P('vp', None), P('dp', None, None), P(None)), check_vma=False)
```

```python
import functools

import jax
import jax.numpy as jnp
from jax import lax
from jax.experimental import pallas as pl
from jax.experimental.pallas import tpu as pltpu
from jax.sharding import PartitionSpec as P

LOGIT_SCALE = 0.0625
EPS = 1e-5
LOG2E = 1.4426950408889634
LN2 = 0.6931471805599453
C2 = LOGIT_SCALE * LOG2E
TB = 256
SPLIT = 9
MIB = 1024 * 1024
NEG = -3e38
MESH = pl.DeviceIdType.MESH


def full(shape):
    return pl.BlockSpec(shape, lambda *_: (0,) * len(shape))


def any_spec():
    return pl.BlockSpec(memory_space=pl.ANY)


def params(limit, **kw):
    return pltpu.CompilerParams(vmem_limit_bytes=limit * MIB, **kw)


def selection(mask_row):
    tokens = mask_row.shape[1]
    rows = lax.broadcasted_iota(jnp.int32, (tokens, tokens), 0)
    cols = lax.broadcasted_iota(jnp.int32, (tokens, tokens), 1)
    upper = jnp.where(rows <= cols, 1.0, 0.0).astype(jnp.bfloat16)
    lhs = jnp.broadcast_to(mask_row, (8, tokens)).astype(jnp.bfloat16)
    rank = jnp.dot(lhs, upper, preferred_element_type=jnp.float32)[0:1]
    hit = (rows.astype(jnp.float32) == rank - 1.0) & (mask_row > 0.0)
    return jnp.where(hit, 1.0, 0.0).astype(jnp.bfloat16)


def normalise(values):
    mean_x = jnp.mean(values, axis=-1, keepdims=True)
    centered = values - mean_x
    variance = jnp.mean(centered * centered, axis=-1, keepdims=True)
    inv_std = lax.rsqrt(variance + EPS)
    return centered * inv_std, inv_std


def prologue(hidden, gain, labels, mask):
    tokens, width = hidden.shape

    def kernel(h_ref, g_ref, l_ref, m_ref, n_ref, nf_ref, hc_ref, meta_ref):
        mask_row = m_ref[...]
        sel = selection(mask_row)
        compact = jnp.dot(sel, h_ref[...], preferred_element_type=jnp.float32)
        hc_ref[...] = compact.astype(jnp.bfloat16)
        x_hat, _ = normalise(compact)
        normed = (g_ref[...] * x_hat).astype(jnp.bfloat16)
        n_ref[...] = normed
        nf_ref[...] = normed.astype(jnp.float32)
        ids = l_ref[...]
        high, mid, low = ids >> 16, (ids >> 8) & 255, ids & 255
        pieces = [p.astype(jnp.float32) for p in (high, mid, low)] + [mask_row]
        stack = jnp.concatenate(pieces + [jnp.zeros((4, tokens), jnp.float32)], axis=0).astype(jnp.bfloat16)
        moved = lax.dot_general(stack, sel, (((1,), (1,)), ((), ())), preferred_element_type=jnp.float32)
        label_row = moved[0:1] * 65536.0 + moved[1:2] * 256.0 + moved[2:3]
        meta_ref[...] = jnp.concatenate([label_row, moved[3:4], jnp.zeros((6, tokens), jnp.float32)], axis=0)

    return pl.pallas_call(
        kernel,
        out_shape=[
            jax.ShapeDtypeStruct((tokens, width), jnp.bfloat16),
            jax.ShapeDtypeStruct((tokens, width), jnp.float32),
            jax.ShapeDtypeStruct((tokens, width), jnp.bfloat16),
            jax.ShapeDtypeStruct((8, tokens), jnp.float32),
        ],
        compiler_params=params(48),
        cost_estimate=pl.CostEstimate(flops=3_000_000_000, bytes_accessed=8_000_000, transcendentals=0),
        name='prologue',
    )(hidden, gain, labels, mask)


def pass_one(count, part, normed, table, z_in, first_block, blocks, tile=2560, slots=6, chunk=256):
    total_blocks = 2 * blocks
    vocab, width = table.shape
    steps = -(-vocab // tile)
    last = vocab - (steps - 1) * tile
    cast = normed.dtype != jnp.bfloat16

    def kernel(nb_ref, _, n_ref, e_ref, *rest):
        if z_in is not None:
            rest = rest[1:]
        if cast:
            z_hbm, st_ref, nout_ref, zbuf, sem = rest
        else:
            z_hbm, st_ref, zbuf, sem = rest
            nout_ref = n_ref
        i = pl.program_id(0)
        nb = nb_ref[0]

        @pl.when(i == 0)
        def _():
            st_ref[:, 0:8, :] = jnp.full((blocks, 8, TB), NEG, jnp.float32)
            st_ref[:, 8:16, :] = jnp.zeros((blocks, 8, TB), jnp.float32)
            if cast:
                nout_ref[...] = n_ref[...].astype(jnp.bfloat16)

        def copy(block, slot, rows, base=0):
            return pltpu.make_async_copy(
                zbuf.at[slot, pl.ds(0, rows)], z_hbm.at[first_block + block, pl.ds(base, rows)], sem.at[slot])

        def body(rows):
            def step(j, _):
                g = i * nb + j
                slot = lax.rem(g, slots)

                @pl.when(g >= slots)
                def _():
                    copy(0, slot, tile).wait()

                run_max = st_ref[j, 0:8, :]
                run_sum = st_ref[j, 8:16, :]
                for lo in range(0, rows, chunk):
                    hi = min(lo + chunk, rows)
                    acc = C2 * lax.dot_general(
                        e_ref[lo:hi], nout_ref[j], (((1,), (1,)), ((), ())), preferred_element_type=jnp.float32)
                    zbuf[slot, lo:hi, :] = acc
                    parts = acc.reshape((hi - lo) // 8, 8, TB)
                    new_max = jnp.maximum(run_max, jnp.max(parts, axis=0))
                    total = jnp.sum(jnp.exp2(parts - new_max[None]), axis=0)
                    run_sum = run_sum * jnp.exp2(run_max - new_max) + total
                    run_max = new_max
                st_ref[j, 0:8, :] = run_max
                st_ref[j, 8:16, :] = run_sum
                copy(j, slot, rows, i * tile).start()
                return 0

            lax.fori_loop(0, nb, step, 0)

        @pl.when(i < steps - 1)
        def _():
            body(tile)

        @pl.when(i == steps - 1)
        def _():
            body(last)
            end = steps * nb
            for q in range(slots):
                slot = lax.rem(end - 1 - q + slots, slots)

                @pl.when(q < nb)
                def _():
                    copy(0, slot, last).wait()

                @pl.when((q >= nb) & (end - 1 - q >= 0))
                def _():
                    copy(0, slot, tile).wait()

    out_shape = [
        jax.ShapeDtypeStruct((total_blocks, vocab, TB), jnp.float32),
        jax.ShapeDtypeStruct((blocks, 16, TB), jnp.float32),
    ]
    out_specs = [any_spec(), full((blocks, 16, TB))]
    if cast:
        out_shape.append(jax.ShapeDtypeStruct((blocks, TB, width), jnp.bfloat16))
        out_specs.append(full((blocks, TB, width)))
    operands = [count, part, normed, table]
    in_specs = [pl.BlockSpec((blocks, TB, width), lambda i, nb, part: (part[0], 0, 0)), pl.BlockSpec((tile, width), lambda i, *_: (i, 0))]
    aliases = {}
    if z_in is not None:
        operands.append(z_in)
        in_specs.append(any_spec())
        aliases = {4: 0}
    return pl.pallas_call(
        kernel,
        grid_spec=pltpu.PrefetchScalarGridSpec(
            num_scalar_prefetch=2, grid=(steps,), in_specs=in_specs, out_specs=out_specs,
            scratch_shapes=[pltpu.VMEM((slots, tile, TB), jnp.float32), pltpu.SemaphoreType.DMA((slots,))]),
        out_shape=out_shape,
        input_output_aliases=aliases,
        compiler_params=params(50),
        cost_estimate=pl.CostEstimate(flops=2 * 2 * TB * vocab * width, bytes_accessed=80_000_000, transcendentals=0),
        name='pass_one',
    )(*operands)


def d_logits(zc, lo, shift, weight, ids):
    scaled = jnp.exp2(zc - shift)
    hit = lax.broadcasted_iota(jnp.int32, zc.shape, 0) == (ids - lo)
    dz = jnp.where(hit, scaled - weight, scaled).astype(jnp.bfloat16)
    picked = jnp.where(hit, zc, 0.0)
    return dz, jnp.sum(picked.reshape(zc.shape[0] // 8, 8, zc.shape[1]), axis=0)


def loop(count, f):
    lax.fori_loop(0, count, lambda j, _: (f(j), 0)[1], 0)


def pass_two_own(count, tokf, toki, table, z, blocks, tile=1280, chunk=256):
    vocab, width = table.shape
    steps = -(-vocab // tile)
    last = vocab - (steps - 1) * tile

    def kernel(nb_ref, tf_ref, ti_ref, e_ref, z_hbm, dz_hbm, dn_ref, zl_ref, za, zb, da, db, zsem, dsem):
        i = pl.program_id(0)
        nb = nb_ref[0]
        zs, ds = (za, zb), (da, db)

        def zcopy(par, j, t, rows):
            return pltpu.make_async_copy(
                z_hbm.at[j, pl.ds(t * tile, rows)], zs[par].at[j, pl.ds(0, rows)], zsem.at[par, j])

        def dcopy(par, j, t, rows):
            return pltpu.make_async_copy(
                ds[par].at[j, pl.ds(0, rows)], dz_hbm.at[j, pl.ds(t * tile, rows)], dsem.at[par, j])

        def make(par, t, j, rows):
            ids = ti_ref[j, 0:1, :] - t * tile
            total = jnp.zeros((8, TB), jnp.float32)
            for lo in range(0, rows, chunk):
                hi = min(lo + chunk, rows)
                dz, picked = d_logits(zs[par][j, lo:hi, :], lo, tf_ref[j, 0:1, :], tf_ref[j, 1:2, :], ids)
                ds[par][j, lo:hi, :] = dz
                total = total + picked
            zl_ref[j] = zl_ref[j] + total

        def product(par, j, rows):
            dn_ref[j] += lax.dot_general(
                ds[par][j, 0:rows, :], e_ref[0:rows, :], (((0,), (0,)), ((), ())), preferred_element_type=jnp.float32)

        @pl.when(i == 0)
        def _():
            dn_ref[...] = jnp.zeros_like(dn_ref)
            zl_ref[...] = jnp.zeros_like(zl_ref)
            loop(nb, lambda j: zcopy(0, j, 0, tile).start())
            loop(nb, lambda j: zcopy(1, j, 1, tile).start())

            def first(j):
                zcopy(0, j, 0, tile).wait()
                make(0, 0, j, tile)
                dcopy(0, j, 0, tile).start()

            loop(nb, first)

        def variant(par, next_rows):
            @pl.when(i + 2 < steps - 1)
            def _():
                loop(nb, lambda j: zcopy(par, j, i + 2, tile).start())

            @pl.when(i + 2 == steps - 1)
            def _():
                loop(nb, lambda j: zcopy(par, j, i + 2, last).start())

            def f(j):
                zcopy(1 - par, j, 0, next_rows).wait()

                @pl.when(i >= 1)
                def _():
                    dcopy(1 - par, j, 0, tile).wait()

                product(par, j, tile)
                make(1 - par, i + 1, j, next_rows)
                dcopy(1 - par, j, i + 1, next_rows).start()

            loop(nb, f)

        end = (steps - 1) % 2
        for par in (0, 1):
            @pl.when((i < steps - 2) & (lax.rem(i, 2) == par))
            def _():
                variant(par, tile)

        @pl.when(i == steps - 2)
        def _():
            variant(1 - end, last)

        @pl.when(i == steps - 1)
        def _():
            def f(j):
                product(end, j, last)
                dcopy(end, j, 0, last).wait()
                dcopy(1 - end, j, 0, tile).wait()

            loop(nb, f)

    halves = tokf.shape[0]
    return pl.pallas_call(
        kernel,
        grid_spec=pltpu.PrefetchScalarGridSpec(
            num_scalar_prefetch=1, grid=(steps,),
            in_specs=[full((halves, 8, TB)), full((halves, 8, TB)), pl.BlockSpec((tile, width), lambda i, *_: (i, 0)),
                      any_spec()],
            out_specs=[any_spec(), full((blocks, TB, width)), full((blocks, 8, TB))],
            scratch_shapes=[pltpu.VMEM((blocks, tile, TB), jnp.float32)] * 2
            + [pltpu.VMEM((blocks, tile, TB), jnp.bfloat16)] * 2 + [pltpu.SemaphoreType.DMA((2, blocks))] * 2),
        out_shape=[jax.ShapeDtypeStruct((blocks, vocab, TB), jnp.bfloat16),
                   jax.ShapeDtypeStruct((blocks, TB, width), jnp.float32), jax.ShapeDtypeStruct((blocks, 8, TB), jnp.float32)],
        compiler_params=params(56),
        cost_estimate=pl.CostEstimate(flops=4 * TB * vocab * width, bytes_accessed=100_000_000, transcendentals=0),
        name='pass_two_own',
    )(count, tokf, toki, table, z)


def pass_two_table(counts, order, tokf, toki, n_own, n_oth, dz_own, z, d_table, after, t0, t1, tile=1280, chunk=256):
    blocks, _, width = n_own.shape
    vocab = z.shape[1]
    steps = -(-vocab // tile)
    last = vocab - (steps - 1) * tile
    halves = 2 * blocks

    def kernel(sc_ref, order_ref, tf_ref, ti_ref, na_ref, nb_ref, dz_hbm, z_hbm, *rest):
        if d_table is not None:
            rest = rest[2:]
        dt_ref, zl_ref, n_ref, za, zb, da, db, zsem, dsem = rest
        i = pl.program_id(0)
        t = i + t0
        own, oth = sc_ref[0], sc_ref[1]
        zs, ds = (za, zb), (da, db)

        def zcopy(par, j, tile_id, rows):
            return pltpu.make_async_copy(
                z_hbm.at[blocks + j, pl.ds(tile_id * tile, rows)], zs[par].at[j, pl.ds(0, rows)], zsem.at[par, j])

        def dcopy(par, j, tile_id, rows):
            return pltpu.make_async_copy(
                dz_hbm.at[j, pl.ds(tile_id * tile, rows)], ds[par].at[j, pl.ds(0, rows)], dsem.at[par, j])

        def load(copy, count, par, tile_id):
            @pl.when((tile_id < t1) & (tile_id < steps - 1))
            def _():
                loop(count, lambda j: copy(par, j, tile_id, tile).start())

            @pl.when((tile_id < t1) & (tile_id == steps - 1))
            def _():
                loop(count, lambda j: copy(par, j, tile_id, last).start())

        def arrive(copy, count, par, tile_id):
            @pl.when((tile_id < t1) & (tile_id < steps - 1))
            def _():
                loop(count, lambda j: copy(par, j, 0, tile).wait())

            @pl.when((tile_id < t1) & (tile_id == steps - 1))
            def _():
                loop(count, lambda j: copy(par, j, 0, last).wait())

        def make(par, tile_id, j):
            ids = ti_ref[blocks + j, 0:1, :] - tile_id * tile
            total = jnp.zeros((8, TB), jnp.float32)
            for lo in range(0, tile, chunk):
                hi = min(lo + chunk, tile)
                dz, picked = d_logits(
                    zs[par][j, lo:hi, :], lo, tf_ref[blocks + j, 0:1, :], tf_ref[blocks + j, 1:2, :], ids)
                ds[par][blocks + j, lo:hi, :] = dz
                total = total + picked
            zl_ref[j] = zl_ref[j] + jnp.where(tile_id < t1, total, 0.0)

        def product(par, j, first):
            block = order_ref[j]
            part = jnp.dot(ds[par][block], n_ref[block], preferred_element_type=jnp.float32)
            if first:
                dt_ref[...] = part
            else:
                dt_ref[...] += part

        @pl.when(i == 0)
        def _():
            zl_ref[...] = jnp.zeros_like(zl_ref)
            load(zcopy, oth, 0, t0)
            load(dcopy, own, 0, t0)
            load(zcopy, oth, 1, t0 + 1)
            n_ref[0:blocks] = na_ref[...]
            n_ref[blocks:] = nb_ref[...]
            arrive(zcopy, oth, 0, t0)
            loop(oth, lambda j: make(0, t0, j))

        def variant(par):
            arrive(dcopy, own, par, t)
            arrive(zcopy, oth, 1 - par, t + 1)
            load(zcopy, oth, par, t + 2)
            load(dcopy, own, 1 - par, t + 1)
            product(par, 0, True)
            make(1 - par, t + 1, 0)

            def both(j, _):
                product(par, j, False)
                make(1 - par, t + 1, j)
                return 0

            def single(j, _):
                product(par, j, False)
                return 0

            lax.fori_loop(1, oth, both, 0)
            lax.fori_loop(oth, own + oth, single, 0)

        for par in (0, 1):
            @pl.when(lax.rem(i, 2) == par)
            def _():
                variant(par)

    operands = [counts, order, tokf, toki, n_own, n_oth, dz_own, z]
    in_specs = [full((halves, 8, TB)), full((halves, 8, TB)), full((blocks, TB, width)), full((blocks, TB, width)),
                any_spec(), any_spec()]
    aliases = {}
    if d_table is not None:
        operands += [d_table, after]
        in_specs += [any_spec(), any_spec()]
        aliases = {8: 0}
    return pl.pallas_call(
        kernel,
        grid_spec=pltpu.PrefetchScalarGridSpec(
            num_scalar_prefetch=2, grid=(t1 - t0,), in_specs=in_specs,
            out_specs=[pl.BlockSpec((tile, width), lambda i, *_: (i + t0, 0)), full((blocks, 8, TB))],
            scratch_shapes=[pltpu.VMEM((halves, TB, width), jnp.bfloat16)]
            + [pltpu.VMEM((blocks, tile, TB), jnp.float32)] * 2 + [pltpu.VMEM((halves, tile, TB), jnp.bfloat16)] * 2
            + [pltpu.SemaphoreType.DMA((2, blocks))] * 2),
        out_shape=[jax.ShapeDtypeStruct((vocab, width), jnp.float32), jax.ShapeDtypeStruct((blocks, 8, TB), jnp.float32)],
        input_output_aliases=aliases,
        compiler_params=params(52),
        cost_estimate=pl.CostEstimate(
            flops=8 * TB * vocab * width * (t1 - t0) // steps, bytes_accessed=100_000_000, transcendentals=0),
        name='pass_two_table',
    )(*operands)


def all_to_peers(buf, send_sem, recv_sem, peers):
    me, ids = peers
    copies = []
    for r, (target, _) in enumerate(ids):
        copies.append(pltpu.make_async_remote_copy(
            src_ref=buf.at[me], dst_ref=buf.at[me], send_sem=send_sem.at[r], recv_sem=recv_sem.at[r],
            device_id=target, device_id_type=MESH))
    for c in copies:
        c.start()
    for c in copies:
        c.wait()


def greet(ids):
    barrier = pltpu.get_barrier_semaphore()
    for target, _ in ids:
        pl.semaphore_signal(barrier, inc=1, device_id=target, device_id_type=MESH)
    pl.semaphore_wait(barrier, len(ids))


def combine_stats(st_own, st_oth, mask_own, mask_oth, vp):
    blocks = st_own.shape[0]
    rows = 2 * blocks

    def kernel(a_ref, b_ref, ma_ref, mb_ref, tf_ref, sum_ref, buf, send_sem, recv_sem):
        me = lax.axis_index('vp')
        dp = lax.axis_index('dp')
        ids = [((dp, lax.rem(me + r, vp)), None) for r in range(1, vp)]
        buf[me] = jnp.zeros((16, TB), jnp.float32)
        for k in range(rows):
            st = (a_ref if k < blocks else b_ref)[k % blocks]
            top = jnp.max(st[0:8], axis=0, keepdims=True)
            total = jnp.sum(st[8:16] * jnp.exp2(st[0:8] - top), axis=0, keepdims=True)
            buf[me, k:k + 1, :] = top
            buf[me, 8 + k:9 + k, :] = total
        greet(ids)
        all_to_peers(buf, send_sem, recv_sem, (me, ids))
        top = buf[0, 0:8, :]
        for k in range(1, vp):
            top = jnp.maximum(top, buf[k, 0:8, :])
        total = jnp.zeros_like(top)
        for k in range(vp):
            total = total + buf[k, 8:16, :] * jnp.exp2(buf[k, 0:8, :] - top)
        masks = jnp.concatenate([ma_ref[...], mb_ref[...], jnp.zeros((8 - rows, TB), jnp.float32)], axis=0)
        log_norm = top + jnp.log2(total)
        count = jnp.sum(masks)
        weight = masks * (LOGIT_SCALE / count)
        shift = log_norm - jnp.log2(weight)
        for k in range(rows):
            tf_ref[k] = jnp.concatenate(
                [shift[k:k + 1], weight[k:k + 1], jnp.zeros((6, TB), jnp.float32)], axis=0)
        kept = jnp.where(masks > 0.0, log_norm * LN2, 0.0)
        both = jnp.sum(kept[0:blocks]) + jnp.sum(kept[blocks:rows])
        sum_ref[...] = jnp.full((8, 128), both / count, jnp.float32)

    return pl.pallas_call(
        kernel,
        out_shape=[jax.ShapeDtypeStruct((rows, 8, TB), jnp.float32), jax.ShapeDtypeStruct((8, 128), jnp.float32)],
        in_specs=[pl.BlockSpec(memory_space=pltpu.VMEM)] * 4,
        out_specs=[pl.BlockSpec(memory_space=pltpu.VMEM)] * 2,
        scratch_shapes=[pltpu.VMEM((vp, 16, TB), jnp.float32), pltpu.SemaphoreType.DMA((vp - 1,)),
                        pltpu.SemaphoreType.DMA((vp - 1,))],
        compiler_params=pltpu.CompilerParams(collective_id=0, has_side_effects=True),
        name='combine_stats',
    )(st_own, st_oth, mask_own, mask_oth)


def norm_back(d_normed, compact, gain, after):
    tokens, width = d_normed.shape

    def kernel(dn_ref, h_ref, g_ref, _, dh_ref, dg_ref):
        dn = dn_ref[...]
        x_hat, inv_std = normalise(h_ref[...].astype(jnp.float32))
        scaled = dn * g_ref[...]
        mean_one = jnp.mean(scaled, axis=-1, keepdims=True)
        mean_two = jnp.mean(scaled * x_hat, axis=-1, keepdims=True)
        grad = (inv_std * (scaled - mean_one - x_hat * mean_two)).astype(jnp.bfloat16)
        dh_ref[...] = grad.astype(jnp.float32)
        dg_ref[...] = jnp.sum((dn * x_hat).reshape(tokens // 8, 8, width), axis=0)

    return pl.pallas_call(
        kernel,
        out_shape=[jax.ShapeDtypeStruct((tokens, width), jnp.float32), jax.ShapeDtypeStruct((8, width), jnp.float32)],
        in_specs=[pl.BlockSpec(memory_space=pltpu.VMEM)] * 3 + [any_spec()],
        name='norm_back',
    )(d_normed, compact, gain, after)


def total_gain(partial, picked, masks, dp_size, vp):
    width = partial.shape[1]
    group = dp_size * vp
    gain_rows = width // 128
    rows = gain_rows + 8

    def kernel(p_ref, z_ref, m_ref, dg_ref, zl_ref, buf, send_sem, recv_sem):
        me = lax.axis_index('dp') * vp + lax.axis_index('vp')
        ids = []
        for r in range(1, group):
            other = lax.rem(me + r, group)
            ids.append(((lax.div(other, vp), lax.rem(other, vp)), None))
        total = jnp.sum(p_ref[...], axis=0, keepdims=True)
        for k in range(gain_rows):
            buf[me, k:k + 1, :] = total[:, k * 128:(k + 1) * 128]
        masks = m_ref[...]
        kept = jnp.where(masks > 0.0, jnp.sum(z_ref[...], axis=1), 0.0)
        half = kept.shape[0] // 2
        both = jnp.sum(kept[:half]) + jnp.sum(kept[half:])
        buf[me, gain_rows:, :] = jnp.full((8, 128), both * LN2 / jnp.sum(masks), jnp.float32)
        greet(ids)
        all_to_peers(buf, send_sem, recv_sem, (me, ids))
        total = buf[0]
        for k in range(1, group):
            total = total + buf[k]
        dg_ref[...] = total[:gain_rows]
        zl_ref[...] = total[gain_rows:] * (1.0 / dp_size)

    return pl.pallas_call(
        kernel,
        out_shape=[jax.ShapeDtypeStruct((gain_rows, 128), jnp.float32), jax.ShapeDtypeStruct((8, 128), jnp.float32)],
        in_specs=[pl.BlockSpec(memory_space=pltpu.VMEM)] * 3,
        out_specs=[pl.BlockSpec(memory_space=pltpu.VMEM)] * 2,
        scratch_shapes=[pltpu.VMEM((group, rows, 128), jnp.float32), pltpu.SemaphoreType.DMA((group - 1,)),
                        pltpu.SemaphoreType.DMA((group - 1,))],
        compiler_params=pltpu.CompilerParams(collective_id=1, has_side_effects=True),
        name='total_gain',
    )(partial, picked, masks)


def scatter_tokens(grads, mask):
    tokens, width = grads.shape

    def kernel(g_ref, m_ref, o_ref):
        sel = selection(m_ref[...])
        o_ref[...] = lax.dot_general(
            sel, g_ref[...].astype(jnp.bfloat16), (((0,), (0,)), ((), ())), preferred_element_type=jnp.float32).astype(jnp.bfloat16)

    return pl.pallas_call(
        kernel, out_shape=jax.ShapeDtypeStruct((tokens, width), jnp.bfloat16), compiler_params=params(48), name='scatter_tokens',
    )(grads, mask)


def solution(mesh):
    dp_size, vp = mesh.shape['dp'], mesh.shape['vp']

    def local_step(hidden, norm_gain, emb_table, labels, tok_mask):
        rows, seq_len, width = hidden.shape
        vocab = emb_table.shape[0]
        tokens = rows * seq_len
        blocks = tokens // TB
        share = tokens // vp
        my_vp = lax.axis_index('vp')
        my_dp = lax.axis_index('dp')
        gain = norm_gain.reshape(1, width)
        mask_row = tok_mask.reshape(1, tokens)
        n_own, n_wide, compact, meta = prologue(hidden.reshape(tokens, width), gain, labels.reshape(1, tokens), mask_row)
        swap = [(0, 1), (1, 0)]
        meta_oth = lax.ppermute(meta, 'dp', swap)
        piece = lax.dynamic_slice_in_dim(n_wide, my_vp * share, share, 0)
        n_wide = lax.all_gather(piece, ('dp', 'vp'), axis=0, tiled=True).reshape(dp_size * blocks, TB, width)
        n_own = n_own.reshape(blocks, TB, width)

        def block_count(m):
            return lax.div(jnp.sum(m[1]).astype(jnp.int32) + (TB - 1), TB)

        nb_own, nb_oth = block_count(meta), block_count(meta_oth)
        z, st_own = pass_one(nb_own[None], jnp.zeros((1,), jnp.int32), n_own, emb_table, None, 0, blocks)
        z, st_oth, n_oth = pass_one(nb_oth[None], (1 - my_dp)[None], n_wide, emb_table, z, blocks, blocks)
        mask_own, mask_oth = meta[1].reshape(blocks, TB), meta_oth[1].reshape(blocks, TB)
        tokf, lse_sum = combine_stats(st_own, st_oth, mask_own, mask_oth, vp)
        ids = jnp.concatenate([meta[0], meta_oth[0]]).astype(jnp.int32).reshape(2 * blocks, 1, TB) - my_vp * vocab
        ids = jnp.where((ids >= 0) & (ids < vocab), ids, -vocab)
        toki = jnp.broadcast_to(ids, (2 * blocks, 8, TB))
        j = jnp.arange(2 * blocks, dtype=jnp.int32)
        first = jnp.where(my_dp == 0, nb_own, nb_oth)
        in_first = j < first
        is_own = in_first == (my_dp == 0)
        local = jnp.where(in_first, j, j - first)
        order = jnp.clip(jnp.where(is_own, local, local + blocks), 0, 2 * blocks - 1)
        counts = jnp.stack([nb_own, nb_oth])
        dz_own, d_part, picked = pass_two_own(nb_own[None], tokf, toki, emb_table, z, blocks)
        d_share = lax.psum_scatter(d_part.reshape(tokens, width), 'vp', scatter_dimension=0, tiled=True)
        args = (counts, order, tokf, toki, n_own, n_oth, dz_own, z)
        steps, cut = -(-vocab // 1280), SPLIT
        d_table, picked_a = pass_two_table(*args, None, None, 0, cut)
        mine = lax.dynamic_slice_in_dim(compact, my_vp * share, share, 0)
        grads, gain_part = norm_back(d_share, mine, gain, picked_a)
        d_table, picked_b = pass_two_table(*args, d_table, gain_part, cut, steps)
        all_grads = lax.all_gather(grads, 'vp', axis=0, tiled=True)
        d_gain, label_sum = total_gain(gain_part, jnp.concatenate([picked, picked_a + picked_b]), jnp.concatenate([mask_own, mask_oth]), dp_size, vp)
        d_hidden = scatter_tokens(all_grads, mask_row)
        loss = lse_sum[0, 0] - label_sum[0, 0]
        return loss, d_table, d_hidden.reshape(rows, seq_len, width), d_gain.reshape(width)

    return jax.shard_map(
        local_step, mesh=mesh,
        in_specs=(P('dp', None, None), P(None), P('vp', None), P('dp', None), P('dp', None)),
        out_specs=(P(), P('vp', None), P('dp', None, None), P(None)), check_vma=False)
```

```python
import functools

import jax
import jax.numpy as jnp
from jax import lax
from jax.experimental import pallas as pl
from jax.experimental.pallas import tpu as pltpu
from jax.sharding import PartitionSpec as P

LOGIT_SCALE = 0.0625
EPS = 1e-5
LOG2E = 1.4426950408889634
LN2 = 0.6931471805599453
C2 = LOGIT_SCALE * LOG2E
TB = 256
SPLIT = 9
MIB = 1024 * 1024
NEG = -3e38
MESH = pl.DeviceIdType.MESH


def full(shape):
    return pl.BlockSpec(shape, lambda *_: (0,) * len(shape))


def any_spec():
    return pl.BlockSpec(memory_space=pl.ANY)


def params(limit, **kw):
    return pltpu.CompilerParams(vmem_limit_bytes=limit * MIB, **kw)


def selection(mask_row):
    tokens = mask_row.shape[1]
    rows = lax.broadcasted_iota(jnp.int32, (tokens, tokens), 0)
    cols = lax.broadcasted_iota(jnp.int32, (tokens, tokens), 1)
    upper = jnp.where(rows <= cols, 1.0, 0.0).astype(jnp.bfloat16)
    lhs = jnp.broadcast_to(mask_row, (8, tokens)).astype(jnp.bfloat16)
    rank = jnp.dot(lhs, upper, preferred_element_type=jnp.float32)[0:1]
    hit = (rows.astype(jnp.float32) == rank - 1.0) & (mask_row > 0.0)
    return jnp.where(hit, 1.0, 0.0).astype(jnp.bfloat16)


def normalise(values):
    mean_x = jnp.mean(values, axis=-1, keepdims=True)
    centered = values - mean_x
    variance = jnp.mean(centered * centered, axis=-1, keepdims=True)
    inv_std = lax.rsqrt(variance + EPS)
    return centered * inv_std, inv_std


def prologue(hidden, gain, labels, mask, vp):
    tokens, width = hidden.shape
    share = tokens // vp

    def kernel(h_ref, g_ref, l_ref, m_ref, n_ref, piece_ref, hc_ref, meta_ref, nb_ref, wide_ref):
        mask_row = m_ref[...]
        sel = selection(mask_row)
        compact = jnp.dot(sel, h_ref[...], preferred_element_type=jnp.float32)
        hc_ref[...] = compact.astype(jnp.bfloat16)
        x_hat, _ = normalise(compact)
        normed = (g_ref[...] * x_hat).astype(jnp.bfloat16)
        n_ref[...] = normed
        wide_ref[...] = normed.astype(jnp.float32)
        mine = pl.multiple_of(lax.axis_index('vp') * share, share)
        piece_ref[0:share, :] = wide_ref[pl.ds(mine, share), :]
        ids = l_ref[...]
        high, mid, low = ids >> 16, (ids >> 8) & 255, ids & 255
        pieces = [p.astype(jnp.float32) for p in (high, mid, low)] + [mask_row]
        stack = jnp.concatenate(pieces + [jnp.zeros((4, tokens), jnp.float32)], axis=0).astype(jnp.bfloat16)
        moved = lax.dot_general(stack, sel, (((1,), (1,)), ((), ())), preferred_element_type=jnp.float32)
        label_row = moved[0:1] * 65536.0 + moved[1:2] * 256.0 + moved[2:3]
        meta = jnp.concatenate([label_row, moved[3:4], jnp.zeros((6, tokens), jnp.float32)], axis=0)
        meta_ref[...] = meta
        piece_ref[share:share + 8, 0:tokens] = meta
        piece_ref[share:share + 8, tokens:] = jnp.zeros((8, width - tokens), jnp.float32)
        nb_ref[0] = lax.div(jnp.sum(mask_row).astype(jnp.int32) + (TB - 1), TB)

    return pl.pallas_call(
        kernel,
        out_shape=[
            jax.ShapeDtypeStruct((tokens, width), jnp.bfloat16),
            jax.ShapeDtypeStruct((share + 8, width), jnp.float32),
            jax.ShapeDtypeStruct((tokens, width), jnp.bfloat16),
            jax.ShapeDtypeStruct((8, tokens), jnp.float32),
            jax.ShapeDtypeStruct((1,), jnp.int32),
        ],
        out_specs=[pl.BlockSpec(memory_space=pltpu.VMEM)] * 4 + [pl.BlockSpec(memory_space=pltpu.SMEM)],
        scratch_shapes=[pltpu.VMEM((tokens, width), jnp.float32)],
        compiler_params=params(48),
        cost_estimate=pl.CostEstimate(flops=3_000_000_000, bytes_accessed=8_000_000, transcendentals=0),
        name='prologue',
    )(hidden, gain, labels, mask)


def pass_one(count, part, normed, table, z_in, first_block, blocks, tile=2560, slots=6, chunk=64):
    total_blocks = 2 * blocks
    vocab, width = table.shape
    steps = -(-vocab // tile)
    last = vocab - (steps - 1) * tile
    cast = normed.dtype != jnp.bfloat16
    tokens = blocks * TB
    share = normed.shape[1] - 8
    groups = tokens // share if cast else 1

    def kernel(nb_ref, _, n_ref, e_ref, *rest):
        if z_in is not None:
            rest = rest[1:]
        if cast:
            z_hbm, st_ref, nout_ref, zbuf, sem = rest
        else:
            z_hbm, st_ref, zbuf, sem = rest
            nout_ref = n_ref
        i = pl.program_id(0)
        nb = nb_ref[0]

        @pl.when(i == 0)
        def _():
            st_ref[:, 0:8, :] = jnp.full((blocks, 8, TB), NEG, jnp.float32)
            st_ref[:, 8:16, :] = jnp.zeros((blocks, 8, TB), jnp.float32)
            if cast:
                for k in range(groups):
                    nout_ref[k * share:(k + 1) * share, :] = n_ref[k, 0:share, :].astype(jnp.bfloat16)

        def copy(block, slot, rows, base=0):
            return pltpu.make_async_copy(
                zbuf.at[slot, pl.ds(0, rows)], z_hbm.at[first_block + block, pl.ds(base, rows)], sem.at[slot])

        def body(rows):
            def step(j, _):
                g = i * nb + j
                slot = lax.rem(g, slots)

                @pl.when(g >= slots)
                def _():
                    copy(0, slot, tile).wait()

                run_max = st_ref[j, 0:8, :]
                run_sum = st_ref[j, 8:16, :]
                block = nout_ref[pl.ds(pl.multiple_of(j * TB, TB), TB), :]
                zbuf[slot, 0:rows, :] = C2 * lax.dot_general(
                    e_ref[0:rows], block, (((1,), (1,)), ((), ())), preferred_element_type=jnp.float32)
                for lo in range(0, rows, chunk):
                    hi = min(lo + chunk, rows)
                    parts = zbuf[slot, lo:hi, :].reshape((hi - lo) // 8, 8, TB)
                    new_max = jnp.maximum(run_max, jnp.max(parts, axis=0))
                    total = jnp.sum(jnp.exp2(parts - new_max[None]), axis=0)
                    run_sum = run_sum * jnp.exp2(run_max - new_max) + total
                    run_max = new_max
                st_ref[j, 0:8, :] = run_max
                st_ref[j, 8:16, :] = run_sum
                copy(j, slot, rows, i * tile).start()
                return 0

            lax.fori_loop(0, nb, step, 0)

        @pl.when(i < steps - 1)
        def _():
            body(tile)

        @pl.when(i == steps - 1)
        def _():
            body(last)
            end = steps * nb
            for q in range(slots):
                slot = lax.rem(end - 1 - q + slots, slots)

                @pl.when(q < nb)
                def _():
                    copy(0, slot, last).wait()

                @pl.when((q >= nb) & (end - 1 - q >= 0))
                def _():
                    copy(0, slot, tile).wait()

    out_shape = [
        jax.ShapeDtypeStruct((total_blocks, vocab, TB), jnp.float32),
        jax.ShapeDtypeStruct((blocks, 16, TB), jnp.float32),
    ]
    out_specs = [any_spec(), full((blocks, 16, TB))]
    if cast:
        out_shape.append(jax.ShapeDtypeStruct((tokens, width), jnp.bfloat16))
        out_specs.append(full((tokens, width)))
        n_spec = pl.BlockSpec((groups, share + 8, width), lambda i, nb, part: (part[0], 0, 0))
    else:
        n_spec = full((tokens, width))
    operands = [count, part, normed, table]
    in_specs = [n_spec, pl.BlockSpec((tile, width), lambda i, *_: (i, 0))]
    aliases = {}
    if z_in is not None:
        operands.append(z_in)
        in_specs.append(any_spec())
        aliases = {4: 0}
    return pl.pallas_call(
        kernel,
        grid_spec=pltpu.PrefetchScalarGridSpec(
            num_scalar_prefetch=2, grid=(steps,), in_specs=in_specs, out_specs=out_specs,
            scratch_shapes=[pltpu.VMEM((slots, tile, TB), jnp.float32), pltpu.SemaphoreType.DMA((slots,))]),
        out_shape=out_shape,
        input_output_aliases=aliases,
        compiler_params=params(50),
        cost_estimate=pl.CostEstimate(flops=2 * 2 * TB * vocab * width, bytes_accessed=80_000_000, transcendentals=0),
        name='pass_one',
    )(*operands)


def d_logits(zc, lo, shift, weight, ids):
    scaled = jnp.exp2(zc - shift)
    hit = lax.broadcasted_iota(jnp.int32, zc.shape, 0) == (ids - lo)
    dz = jnp.where(hit, scaled - weight, scaled).astype(jnp.bfloat16)
    picked = jnp.where(hit, zc, 0.0)
    return dz, jnp.sum(picked.reshape(zc.shape[0] // 8, 8, zc.shape[1]), axis=0)


def loop(count, f):
    lax.fori_loop(0, count, lambda j, _: (f(j), 0)[1], 0)


def pass_two_own(count, tokf, toki, table, z, blocks, tile=1280, chunk=32):
    vocab, width = table.shape
    steps = -(-vocab // tile)
    last = vocab - (steps - 1) * tile

    def kernel(nb_ref, tf_ref, ti_ref, e_ref, z_hbm, dz_hbm, dn_ref, zl_ref, za, zb, da, db, zsem, dsem):
        i = pl.program_id(0)
        nb = nb_ref[0]
        zs, ds = (za, zb), (da, db)

        def zcopy(par, j, t, rows):
            return pltpu.make_async_copy(
                z_hbm.at[j, pl.ds(t * tile, rows)], zs[par].at[j, pl.ds(0, rows)], zsem.at[par, j])

        def dcopy(par, j, t, rows):
            return pltpu.make_async_copy(
                ds[par].at[j, pl.ds(0, rows)], dz_hbm.at[j, pl.ds(t * tile, rows)], dsem.at[par, j])

        def make(par, t, j, rows):
            ids = ti_ref[j, 0:1, :] - t * tile
            total = jnp.zeros((8, TB), jnp.float32)
            for lo in range(0, rows, chunk):
                hi = min(lo + chunk, rows)
                dz, picked = d_logits(zs[par][j, lo:hi, :], lo, tf_ref[j, 0:1, :], tf_ref[j, 1:2, :], ids)
                ds[par][j, lo:hi, :] = dz
                total = total + picked
            zl_ref[j] = zl_ref[j] + total

        def product(par, j, rows):
            dn_ref[j] += lax.dot_general(
                ds[par][j, 0:rows, :], e_ref[0:rows, :], (((0,), (0,)), ((), ())), preferred_element_type=jnp.float32)

        @pl.when(i == 0)
        def _():
            dn_ref[...] = jnp.zeros_like(dn_ref)
            zl_ref[...] = jnp.zeros_like(zl_ref)
            loop(nb, lambda j: zcopy(0, j, 0, tile).start())
            loop(nb, lambda j: zcopy(1, j, 1, tile).start())

            def first(j):
                zcopy(0, j, 0, tile).wait()
                make(0, 0, j, tile)
                dcopy(0, j, 0, tile).start()

            loop(nb, first)

        def variant(par, next_rows):
            @pl.when(i + 2 < steps - 1)
            def _():
                loop(nb, lambda j: zcopy(par, j, i + 2, tile).start())

            @pl.when(i + 2 == steps - 1)
            def _():
                loop(nb, lambda j: zcopy(par, j, i + 2, last).start())

            def f(j):
                zcopy(1 - par, j, 0, next_rows).wait()

                @pl.when(i >= 1)
                def _():
                    dcopy(1 - par, j, 0, tile).wait()

                product(par, j, tile)
                make(1 - par, i + 1, j, next_rows)
                dcopy(1 - par, j, i + 1, next_rows).start()

            loop(nb, f)

        end = (steps - 1) % 2
        for par in (0, 1):
            @pl.when((i < steps - 2) & (lax.rem(i, 2) == par))
            def _():
                variant(par, tile)

        @pl.when(i == steps - 2)
        def _():
            variant(1 - end, last)

        @pl.when(i == steps - 1)
        def _():
            def f(j):
                product(end, j, last)
                dcopy(end, j, 0, last).wait()
                dcopy(1 - end, j, 0, tile).wait()

            loop(nb, f)

    halves = tokf.shape[0]
    return pl.pallas_call(
        kernel,
        grid_spec=pltpu.PrefetchScalarGridSpec(
            num_scalar_prefetch=1, grid=(steps,),
            in_specs=[full((halves, 8, TB)), full((halves, 8, TB)), pl.BlockSpec((tile, width), lambda i, *_: (i, 0)),
                      any_spec()],
            out_specs=[any_spec(), full((blocks, TB, width)), full((blocks, 8, TB))],
            scratch_shapes=[pltpu.VMEM((blocks, tile, TB), jnp.float32)] * 2
            + [pltpu.VMEM((blocks, tile, TB), jnp.bfloat16)] * 2 + [pltpu.SemaphoreType.DMA((2, blocks))] * 2),
        out_shape=[jax.ShapeDtypeStruct((blocks, vocab, TB), jnp.bfloat16),
                   jax.ShapeDtypeStruct((blocks, TB, width), jnp.float32), jax.ShapeDtypeStruct((blocks, 8, TB), jnp.float32)],
        compiler_params=params(56),
        cost_estimate=pl.CostEstimate(flops=4 * TB * vocab * width, bytes_accessed=100_000_000, transcendentals=0),
        name='pass_two_own',
    )(count, tokf, toki, table, z)


def pass_two_table(counts, order, tokf, toki, n_own, n_oth, dz_own, z, d_table, after, t0, t1, tile=1280, chunk=64, half=640):
    blocks, _, width = n_own.shape
    vocab = z.shape[1]
    steps = -(-vocab // tile)
    last = vocab - (steps - 1) * tile
    halves = 2 * blocks

    def kernel(sc_ref, order_ref, tf_ref, ti_ref, na_ref, nb_ref, dz_hbm, z_hbm, *rest):
        if d_table is not None:
            rest = rest[2:]
        dt_ref, zl_ref, n_ref, za, zb, da, db, zsem, dsem = rest
        i = pl.program_id(0)
        t = i + t0
        own, oth = sc_ref[0], sc_ref[1]
        zs, ds = (za, zb), (da, db)

        def zcopy(par, j, tile_id, rows):
            return pltpu.make_async_copy(
                z_hbm.at[blocks + j, pl.ds(tile_id * tile, rows)], zs[par].at[j, pl.ds(0, rows)], zsem.at[par, j])

        def dcopy(par, j, tile_id, rows):
            return pltpu.make_async_copy(
                dz_hbm.at[j, pl.ds(tile_id * tile, rows)], ds[par].at[j, pl.ds(0, rows)], dsem.at[par, j])

        def load(copy, count, par, tile_id):
            @pl.when((tile_id < t1) & (tile_id < steps - 1))
            def _():
                loop(count, lambda j: copy(par, j, tile_id, tile).start())

            @pl.when((tile_id < t1) & (tile_id == steps - 1))
            def _():
                loop(count, lambda j: copy(par, j, tile_id, last).start())

        def arrive(copy, count, par, tile_id):
            @pl.when((tile_id < t1) & (tile_id < steps - 1))
            def _():
                loop(count, lambda j: copy(par, j, 0, tile).wait())

            @pl.when((tile_id < t1) & (tile_id == steps - 1))
            def _():
                loop(count, lambda j: copy(par, j, 0, last).wait())

        def make(par, tile_id, j, first, end):
            ids = ti_ref[blocks + j, 0:1, :] - tile_id * tile
            total = jnp.zeros((8, TB), jnp.float32)
            for lo in range(first, end, chunk):
                hi = min(lo + chunk, end)
                dz, picked = d_logits(
                    zs[par][j, lo:hi, :], lo, tf_ref[blocks + j, 0:1, :], tf_ref[blocks + j, 1:2, :], ids)
                ds[par][blocks + j, lo:hi, :] = dz
                total = total + picked
            zl_ref[j] = zl_ref[j] + jnp.where(tile_id < t1, total, 0.0)

        def product(par, j, fresh, first, end):
            block = order_ref[j]
            part = jnp.dot(ds[par][block, first:end, :], n_ref[block], preferred_element_type=jnp.float32)
            if fresh:
                dt_ref[first:end, :] = part
            else:
                dt_ref[first:end, :] += part

        def mixed(par, j, fresh):
            for first in range(0, tile, half):
                product(par, j, fresh, first, first + half)
                make(1 - par, t + 1, j, first, first + half)

        @pl.when(i == 0)
        def _():
            zl_ref[...] = jnp.zeros_like(zl_ref)
            load(zcopy, oth, 0, t0)
            load(dcopy, own, 0, t0)
            load(zcopy, oth, 1, t0 + 1)
            n_ref[0:blocks] = na_ref[...]
            n_ref[blocks:] = nb_ref[...]
            arrive(zcopy, oth, 0, t0)
            loop(oth, lambda j: make(0, t0, j, 0, tile))

        def variant(par):
            arrive(dcopy, own, par, t)
            arrive(zcopy, oth, 1 - par, t + 1)
            load(zcopy, oth, par, t + 2)
            load(dcopy, own, 1 - par, t + 1)
            mixed(par, 0, True)

            def both(j, _):
                mixed(par, j, False)
                return 0

            def single(j, _):
                product(par, j, False, 0, tile)
                return 0

            lax.fori_loop(1, oth, both, 0)
            lax.fori_loop(oth, own + oth, single, 0)

        for par in (0, 1):
            @pl.when(lax.rem(i, 2) == par)
            def _():
                variant(par)

    operands = [counts, order, tokf, toki, n_own, n_oth, dz_own, z]
    in_specs = [full((halves, 8, TB)), full((halves, 8, TB)), full((blocks, TB, width)), full((blocks, TB, width)),
                any_spec(), any_spec()]
    aliases = {}
    if d_table is not None:
        operands += [d_table, after]
        in_specs += [any_spec(), any_spec()]
        aliases = {8: 0}
    return pl.pallas_call(
        kernel,
        grid_spec=pltpu.PrefetchScalarGridSpec(
            num_scalar_prefetch=2, grid=(t1 - t0,), in_specs=in_specs,
            out_specs=[pl.BlockSpec((tile, width), lambda i, *_: (i + t0, 0)), full((blocks, 8, TB))],
            scratch_shapes=[pltpu.VMEM((halves, TB, width), jnp.bfloat16)]
            + [pltpu.VMEM((blocks, tile, TB), jnp.float32)] * 2 + [pltpu.VMEM((halves, tile, TB), jnp.bfloat16)] * 2
            + [pltpu.SemaphoreType.DMA((2, blocks))] * 2),
        out_shape=[jax.ShapeDtypeStruct((vocab, width), jnp.float32), jax.ShapeDtypeStruct((blocks, 8, TB), jnp.float32)],
        input_output_aliases=aliases,
        compiler_params=params(52),
        cost_estimate=pl.CostEstimate(
            flops=8 * TB * vocab * width * (t1 - t0) // steps, bytes_accessed=100_000_000, transcendentals=0),
        name='pass_two_table',
    )(*operands)


def all_to_peers(buf, send_sem, recv_sem, peers):
    me, ids = peers
    copies = []
    for r, (target, _) in enumerate(ids):
        copies.append(pltpu.make_async_remote_copy(
            src_ref=buf.at[me], dst_ref=buf.at[me], send_sem=send_sem.at[r], recv_sem=recv_sem.at[r],
            device_id=target, device_id_type=MESH))
    for c in copies:
        c.start()
    return copies


def greet(ids):
    barrier = pltpu.get_barrier_semaphore()
    for target, _ in ids:
        pl.semaphore_signal(barrier, inc=1, device_id=target, device_id_type=MESH)
    pl.semaphore_wait(barrier, len(ids))


def combine_stats(st_own, st_oth, mask_own, mask_oth, vp):
    blocks = st_own.shape[0]
    rows = 2 * blocks

    def kernel(a_ref, b_ref, ma_ref, mb_ref, tf_ref, sum_ref, buf, send_sem, recv_sem):
        me = lax.axis_index('vp')
        dp = lax.axis_index('dp')
        ids = [((dp, lax.rem(me + r, vp)), None) for r in range(1, vp)]
        buf[me] = jnp.zeros((16, TB), jnp.float32)
        for k in range(rows):
            st = (a_ref if k < blocks else b_ref)[k % blocks]
            top = jnp.max(st[0:8], axis=0, keepdims=True)
            total = jnp.sum(st[8:16] * jnp.exp2(st[0:8] - top), axis=0, keepdims=True)
            buf[me, k:k + 1, :] = top
            buf[me, 8 + k:9 + k, :] = total
        greet(ids)
        for c in all_to_peers(buf, send_sem, recv_sem, (me, ids)):
            c.wait()
        top = buf[0, 0:8, :]
        for k in range(1, vp):
            top = jnp.maximum(top, buf[k, 0:8, :])
        total = jnp.zeros_like(top)
        for k in range(vp):
            total = total + buf[k, 8:16, :] * jnp.exp2(buf[k, 0:8, :] - top)
        masks = jnp.concatenate([ma_ref[...], mb_ref[...], jnp.zeros((8 - rows, TB), jnp.float32)], axis=0)
        log_norm = top + jnp.log2(total)
        count = jnp.sum(masks)
        weight = masks * (LOGIT_SCALE / count)
        shift = log_norm - jnp.log2(weight)
        for k in range(rows):
            tf_ref[k] = jnp.concatenate(
                [shift[k:k + 1], weight[k:k + 1], jnp.zeros((6, TB), jnp.float32)], axis=0)
        kept = jnp.where(masks > 0.0, log_norm * LN2, 0.0)
        both = jnp.sum(kept[0:blocks]) + jnp.sum(kept[blocks:rows])
        sum_ref[...] = jnp.full((8, 128), both / count, jnp.float32)

    return pl.pallas_call(
        kernel,
        out_shape=[jax.ShapeDtypeStruct((rows, 8, TB), jnp.float32), jax.ShapeDtypeStruct((8, 128), jnp.float32)],
        in_specs=[pl.BlockSpec(memory_space=pltpu.VMEM)] * 4,
        out_specs=[pl.BlockSpec(memory_space=pltpu.VMEM)] * 2,
        scratch_shapes=[pltpu.VMEM((vp, 16, TB), jnp.float32), pltpu.SemaphoreType.DMA((vp - 1,)),
                        pltpu.SemaphoreType.DMA((vp - 1,))],
        compiler_params=pltpu.CompilerParams(collective_id=0, has_side_effects=True),
        name='combine_stats',
    )(st_own, st_oth, mask_own, mask_oth)


def norm_back(d_normed, compact, gain, after):
    tokens, width = d_normed.shape

    def kernel(dn_ref, h_ref, g_ref, _, dh_ref, dg_ref):
        dn = dn_ref[...]
        x_hat, inv_std = normalise(h_ref[...].astype(jnp.float32))
        scaled = dn * g_ref[...]
        mean_one = jnp.mean(scaled, axis=-1, keepdims=True)
        mean_two = jnp.mean(scaled * x_hat, axis=-1, keepdims=True)
        grad = (inv_std * (scaled - mean_one - x_hat * mean_two)).astype(jnp.bfloat16)
        dh_ref[...] = grad.astype(jnp.float32)
        dg_ref[...] = jnp.sum((dn * x_hat).reshape(tokens // 8, 8, width), axis=0)

    return pl.pallas_call(
        kernel,
        out_shape=[jax.ShapeDtypeStruct((tokens, width), jnp.float32), jax.ShapeDtypeStruct((8, width), jnp.float32)],
        in_specs=[pl.BlockSpec(memory_space=pltpu.VMEM)] * 3 + [any_spec()],
        name='norm_back',
    )(d_normed, compact, gain, after)


def finish(grads, mask, partial, picked, masks, lse_sum, dp_size, vp):
    tokens, width = grads.shape
    group = dp_size * vp
    gain_rows = width // 128
    rows = gain_rows + 8

    def kernel(g_ref, t_ref, p_ref, z_ref, m_ref, s_ref, dh_ref, dg_ref, loss_ref, buf, send_sem, recv_sem):
        me = lax.axis_index('dp') * vp + lax.axis_index('vp')
        ids = []
        for r in range(1, group):
            other = lax.rem(me + r, group)
            ids.append(((lax.div(other, vp), lax.rem(other, vp)), None))
        total = jnp.sum(p_ref[...], axis=0, keepdims=True)
        for k in range(gain_rows):
            buf[me, k:k + 1, :] = total[:, k * 128:(k + 1) * 128]
        masks = m_ref[...]
        kept = jnp.where(masks > 0.0, jnp.sum(z_ref[...], axis=1), 0.0)
        half = kept.shape[0] // 2
        both = jnp.sum(kept[:half]) + jnp.sum(kept[half:])
        buf[me, gain_rows:, :] = jnp.full((8, 128), both * LN2 / jnp.sum(masks), jnp.float32)
        greet(ids)
        copies = all_to_peers(buf, send_sem, recv_sem, (me, ids))
        sel = selection(t_ref[...])
        dh_ref[...] = lax.dot_general(
            sel, g_ref[...].astype(jnp.bfloat16), (((0,), (0,)), ((), ())), preferred_element_type=jnp.float32).astype(jnp.bfloat16)
        for c in copies:
            c.wait()
        total = buf[0]
        for k in range(1, group):
            total = total + buf[k]
        dg_ref[...] = total[:gain_rows]
        loss_ref[...] = s_ref[...] - total[gain_rows:] * (1.0 / dp_size)

    return pl.pallas_call(
        kernel,
        out_shape=[jax.ShapeDtypeStruct((tokens, width), jnp.bfloat16), jax.ShapeDtypeStruct((gain_rows, 128), jnp.float32),
                   jax.ShapeDtypeStruct((8, 128), jnp.float32)],
        in_specs=[pl.BlockSpec(memory_space=pltpu.VMEM)] * 6,
        out_specs=[pl.BlockSpec(memory_space=pltpu.VMEM)] * 3,
        scratch_shapes=[pltpu.VMEM((group, rows, 128), jnp.float32), pltpu.SemaphoreType.DMA((group - 1,)),
                        pltpu.SemaphoreType.DMA((group - 1,))],
        compiler_params=params(48, collective_id=1, has_side_effects=True),
        name='finish',
    )(grads, mask, partial, picked, masks, lse_sum)


def solution(mesh):
    dp_size, vp = mesh.shape['dp'], mesh.shape['vp']

    def local_step(hidden, norm_gain, emb_table, labels, tok_mask):
        rows, seq_len, width = hidden.shape
        vocab = emb_table.shape[0]
        tokens = rows * seq_len
        blocks = tokens // TB
        share = tokens // vp
        my_vp = lax.axis_index('vp')
        my_dp = lax.axis_index('dp')
        gain = norm_gain.reshape(1, width)
        mask_row = tok_mask.reshape(1, tokens)
        n_own, piece, compact, meta, nb_own = prologue(
            hidden.reshape(tokens, width), gain, labels.reshape(1, tokens), mask_row, vp)
        pieces = lax.all_gather(piece, ('dp', 'vp'), axis=0)
        z, st_own = pass_one(nb_own, jnp.zeros((1,), jnp.int32), n_own, emb_table, None, 0, blocks)
        meta_oth = lax.dynamic_slice(pieces, ((1 - my_dp) * vp, share, 0), (1, 2, tokens))[0]
        nb_own = nb_own[0]
        nb_oth = lax.div(jnp.sum(meta_oth[1]).astype(jnp.int32) + (TB - 1), TB)
        z, st_oth, n_oth = pass_one(nb_oth[None], (1 - my_dp)[None], pieces, emb_table, z, blocks, blocks)
        n_own, n_oth = n_own.reshape(blocks, TB, width), n_oth.reshape(blocks, TB, width)
        mask_own, mask_oth = meta[1].reshape(blocks, TB), meta_oth[1].reshape(blocks, TB)
        tokf, lse_sum = combine_stats(st_own, st_oth, mask_own, mask_oth, vp)
        ids = jnp.concatenate([meta[0], meta_oth[0]]).astype(jnp.int32).reshape(2 * blocks, 1, TB) - my_vp * vocab
        ids = jnp.where((ids >= 0) & (ids < vocab), ids, -vocab)
        toki = jnp.broadcast_to(ids, (2 * blocks, 8, TB))
        j = jnp.arange(2 * blocks, dtype=jnp.int32)
        first = jnp.where(my_dp == 0, nb_own, nb_oth)
        in_first = j < first
        is_own = in_first == (my_dp == 0)
        local = jnp.where(in_first, j, j - first)
        order = jnp.clip(jnp.where(is_own, local, local + blocks), 0, 2 * blocks - 1)
        counts = jnp.stack([nb_own, nb_oth])
        dz_own, d_part, picked = pass_two_own(nb_own[None], tokf, toki, emb_table, z, blocks)
        d_share = lax.psum_scatter(d_part.reshape(tokens, width), 'vp', scatter_dimension=0, tiled=True)
        args = (counts, order, tokf, toki, n_own, n_oth, dz_own, z)
        steps, cut = -(-vocab // 1280), SPLIT
        d_table, picked_a = pass_two_table(*args, None, None, 0, cut)
        mine = lax.dynamic_slice_in_dim(compact, my_vp * share, share, 0)
        grads, gain_part = norm_back(d_share, mine, gain, picked_a)
        d_table, picked_b = pass_two_table(*args, d_table, gain_part, cut, steps)
        all_grads = lax.all_gather(grads, 'vp', axis=0, tiled=True)
        d_hidden, d_gain, loss = finish(
            all_grads, mask_row, gain_part, jnp.concatenate([picked, picked_a + picked_b]),
            jnp.concatenate([mask_own, mask_oth]), lse_sum, dp_size, vp)
        return loss[0, 0], d_table, d_hidden.reshape(rows, seq_len, width), d_gain.reshape(width)

    return jax.shard_map(
        local_step, mesh=mesh,
        in_specs=(P('dp', None, None), P(None), P('vp', None), P('dp', None), P('dp', None)),
        out_specs=(P(), P('vp', None), P('dp', None, None), P(None)), check_vma=False)
```

```python
import functools

import jax
import jax.numpy as jnp
from jax import lax
from jax.experimental import pallas as pl
from jax.experimental.pallas import tpu as pltpu
from jax.sharding import PartitionSpec as P

LOGIT_SCALE = 0.0625
EPS = 1e-5
LOG2E = 1.4426950408889634
LN2 = 0.6931471805599453
C2 = LOGIT_SCALE * LOG2E
TB = 256
SPLIT = 9
MIB = 1024 * 1024
NEG = -3e38
MESH = pl.DeviceIdType.MESH


def full(shape):
    return pl.BlockSpec(shape, lambda *_: (0,) * len(shape))


def any_spec():
    return pl.BlockSpec(memory_space=pl.ANY)


def params(limit, **kw):
    return pltpu.CompilerParams(vmem_limit_bytes=limit * MIB, **kw)


def selection(mask_row):
    tokens = mask_row.shape[1]
    rows = lax.broadcasted_iota(jnp.int32, (tokens, tokens), 0)
    cols = lax.broadcasted_iota(jnp.int32, (tokens, tokens), 1)
    upper = jnp.where(rows <= cols, 1.0, 0.0).astype(jnp.bfloat16)
    lhs = jnp.broadcast_to(mask_row, (8, tokens)).astype(jnp.bfloat16)
    rank = jnp.dot(lhs, upper, preferred_element_type=jnp.float32)[0:1]
    hit = (rows.astype(jnp.float32) == rank - 1.0) & (mask_row > 0.0)
    return jnp.where(hit, 1.0, 0.0).astype(jnp.bfloat16)


def one_row(ref):
    return jnp.concatenate([ref[r:r + 1, :] for r in range(ref.shape[0])], axis=1)


def normalise(values):
    mean_x = jnp.mean(values, axis=-1, keepdims=True)
    centered = values - mean_x
    variance = jnp.mean(centered * centered, axis=-1, keepdims=True)
    inv_std = lax.rsqrt(variance + EPS)
    return centered * inv_std, inv_std


def prologue(hidden, gain, labels, mask, vp):
    tokens, width = hidden.shape
    share = tokens // vp

    def kernel(h_hbm, g_hbm, l_hbm, m_hbm, n_ref, piece_ref, hc_ref, meta_ref, nb_ref, wide_ref, h_ref, g_ref, l_ref, m_ref,
               sem):
        pairs = ((h_hbm, h_ref), (g_hbm, g_ref), (l_hbm, l_ref), (m_hbm, m_ref))
        copies = [pltpu.make_async_copy(src, dst, sem.at[k]) for k, (src, dst) in enumerate(pairs)]
        for c in copies:
            c.start()
        for c in copies:
            c.wait()
        mask_row = one_row(m_ref)
        sel = selection(mask_row)
        compact = jnp.dot(sel, h_ref[...], preferred_element_type=jnp.float32)
        mine = pl.multiple_of(lax.axis_index('vp') * share, share)
        wide_ref[0] = compact
        hc_ref[...] = wide_ref[0, pl.ds(mine, share), :]
        x_hat, _ = normalise(compact)
        normed = (g_ref[...] * x_hat).astype(jnp.bfloat16)
        n_ref[...] = normed
        wide_ref[1] = normed.astype(jnp.float32)
        piece_ref[0:share, :] = wide_ref[1, pl.ds(mine, share), :]
        ids = one_row(l_ref)
        high, mid, low = ids >> 16, (ids >> 8) & 255, ids & 255
        pieces = [p.astype(jnp.float32) for p in (high, mid, low)] + [mask_row]
        stack = jnp.concatenate(pieces + [jnp.zeros((4, tokens), jnp.float32)], axis=0).astype(jnp.bfloat16)
        moved = lax.dot_general(stack, sel, (((1,), (1,)), ((), ())), preferred_element_type=jnp.float32)
        label_row = moved[0:1] * 65536.0 + moved[1:2] * 256.0 + moved[2:3]
        meta = jnp.concatenate([label_row, moved[3:4], jnp.zeros((6, tokens), jnp.float32)], axis=0)
        meta_ref[...] = meta
        piece_ref[share:share + 8, 0:tokens] = meta
        piece_ref[share:share + 8, tokens:] = jnp.zeros((8, width - tokens), jnp.float32)
        nb_ref[0] = lax.div(jnp.sum(mask_row).astype(jnp.int32) + (TB - 1), TB)

    return pl.pallas_call(
        kernel,
        out_shape=[
            jax.ShapeDtypeStruct((tokens, width), jnp.bfloat16),
            jax.ShapeDtypeStruct((share + 8, width), jnp.float32),
            jax.ShapeDtypeStruct((share, width), jnp.float32),
            jax.ShapeDtypeStruct((8, tokens), jnp.float32),
            jax.ShapeDtypeStruct((1,), jnp.int32),
        ],
        out_specs=[pl.BlockSpec(memory_space=pltpu.VMEM)] * 4 + [pl.BlockSpec(memory_space=pltpu.SMEM)],
        in_specs=[pl.BlockSpec(memory_space=pltpu.HBM)] * 4,
        scratch_shapes=[pltpu.VMEM((2, tokens, width), jnp.float32)]
        + [pltpu.VMEM(a.shape, a.dtype) for a in (hidden, gain, labels, mask)] + [pltpu.SemaphoreType.DMA((4,))],
        compiler_params=params(48),
        cost_estimate=pl.CostEstimate(flops=3_000_000_000, bytes_accessed=8_000_000, transcendentals=0),
        name='prologue',
    )(hidden, gain, labels, mask)


def pass_one(count, part, normed, table, z_in, first_block, blocks, tile=2560, slots=6, chunk=64):
    total_blocks = 2 * blocks
    vocab, width = table.shape
    steps = -(-vocab // tile)
    last = vocab - (steps - 1) * tile
    cast = normed.dtype != jnp.bfloat16
    tokens = blocks * TB
    share = normed.shape[1] - 8
    groups = tokens // share if cast else 1

    def kernel(nb_ref, _, n_ref, e_ref, *rest):
        if z_in is not None:
            rest = rest[1:]
        if cast:
            z_hbm, st_ref, nout_ref, zbuf, sem = rest
        else:
            z_hbm, st_ref, zbuf, sem = rest
            nout_ref = n_ref
        i = pl.program_id(0)
        nb = nb_ref[0]

        @pl.when(i == 0)
        def _():
            st_ref[:, 0:8, :] = jnp.full((blocks, 8, TB), NEG, jnp.float32)
            st_ref[:, 8:16, :] = jnp.zeros((blocks, 8, TB), jnp.float32)
            if cast:
                for k in range(groups):
                    nout_ref[k * share:(k + 1) * share, :] = n_ref[k, 0:share, :].astype(jnp.bfloat16)

        def copy(block, slot, rows, base=0):
            return pltpu.make_async_copy(
                zbuf.at[slot, pl.ds(0, rows)], z_hbm.at[first_block + block, pl.ds(base, rows)], sem.at[slot])

        def body(rows):
            def step(j, _):
                g = i * nb + j
                slot = lax.rem(g, slots)

                @pl.when(g >= slots)
                def _():
                    copy(0, slot, tile).wait()

                run_max = st_ref[j, 0:8, :]
                run_sum = st_ref[j, 8:16, :]
                block = nout_ref[pl.ds(pl.multiple_of(j * TB, TB), TB), :]
                zbuf[slot, 0:rows, :] = C2 * lax.dot_general(
                    e_ref[0:rows], block, (((1,), (1,)), ((), ())), preferred_element_type=jnp.float32)
                for lo in range(0, rows, chunk):
                    hi = min(lo + chunk, rows)
                    parts = zbuf[slot, lo:hi, :].reshape((hi - lo) // 8, 8, TB)
                    new_max = jnp.maximum(run_max, jnp.max(parts, axis=0))
                    total = jnp.sum(jnp.exp2(parts - new_max[None]), axis=0)
                    run_sum = run_sum * jnp.exp2(run_max - new_max) + total
                    run_max = new_max
                st_ref[j, 0:8, :] = run_max
                st_ref[j, 8:16, :] = run_sum
                copy(j, slot, rows, i * tile).start()
                return 0

            lax.fori_loop(0, nb, step, 0)

        @pl.when(i < steps - 1)
        def _():
            body(tile)

        @pl.when(i == steps - 1)
        def _():
            body(last)
            end = steps * nb
            for q in range(slots):
                slot = lax.rem(end - 1 - q + slots, slots)

                @pl.when(q < nb)
                def _():
                    copy(0, slot, last).wait()

                @pl.when((q >= nb) & (end - 1 - q >= 0))
                def _():
                    copy(0, slot, tile).wait()

    out_shape = [
        jax.ShapeDtypeStruct((total_blocks, vocab, TB), jnp.float32),
        jax.ShapeDtypeStruct((blocks, 16, TB), jnp.float32),
    ]
    out_specs = [any_spec(), full((blocks, 16, TB))]
    if cast:
        out_shape.append(jax.ShapeDtypeStruct((tokens, width), jnp.bfloat16))
        out_specs.append(full((tokens, width)))
        n_spec = pl.BlockSpec((groups, share + 8, width), lambda i, nb, part: (part[0], 0, 0))
    else:
        n_spec = full((tokens, width))
    operands = [count, part, normed, table]
    in_specs = [n_spec, pl.BlockSpec((tile, width), lambda i, *_: (i, 0))]
    aliases = {}
    if z_in is not None:
        operands.append(z_in)
        in_specs.append(any_spec())
        aliases = {4: 0}
    return pl.pallas_call(
        kernel,
        grid_spec=pltpu.PrefetchScalarGridSpec(
            num_scalar_prefetch=2, grid=(steps,), in_specs=in_specs, out_specs=out_specs,
            scratch_shapes=[pltpu.VMEM((slots, tile, TB), jnp.float32), pltpu.SemaphoreType.DMA((slots,))]),
        out_shape=out_shape,
        input_output_aliases=aliases,
        compiler_params=params(50),
        cost_estimate=pl.CostEstimate(flops=2 * 2 * TB * vocab * width, bytes_accessed=80_000_000, transcendentals=0),
        name='pass_one',
    )(*operands)


def d_logits(zc, lo, shift, weight, ids):
    scaled = jnp.exp2(zc - shift)
    hit = lax.broadcasted_iota(jnp.int32, zc.shape, 0) == (ids - lo)
    dz = jnp.where(hit, scaled - weight, scaled).astype(jnp.bfloat16)
    picked = jnp.where(hit, zc, 0.0)
    return dz, jnp.sum(picked.reshape(zc.shape[0] // 8, 8, zc.shape[1]), axis=0)


def loop(count, f):
    lax.fori_loop(0, count, lambda j, _: (f(j), 0)[1], 0)


def pass_two_own(count, tokf, toki, table, z, blocks, tile=1280, chunk=32):
    vocab, width = table.shape
    steps = -(-vocab // tile)
    last = vocab - (steps - 1) * tile

    def kernel(nb_ref, tf_ref, ti_ref, e_ref, z_hbm, dz_hbm, dn_ref, zl_ref, za, zb, da, db, zsem, dsem):
        i = pl.program_id(0)
        nb = nb_ref[0]
        zs, ds = (za, zb), (da, db)

        def zcopy(par, j, t, rows):
            return pltpu.make_async_copy(
                z_hbm.at[j, pl.ds(t * tile, rows)], zs[par].at[j, pl.ds(0, rows)], zsem.at[par, j])

        def dcopy(par, j, t, rows):
            return pltpu.make_async_copy(
                ds[par].at[j, pl.ds(0, rows)], dz_hbm.at[j, pl.ds(t * tile, rows)], dsem.at[par, j])

        def make(par, t, j, rows):
            ids = ti_ref[j, 0:1, :] - t * tile
            total = jnp.zeros((8, TB), jnp.float32)
            for lo in range(0, rows, chunk):
                hi = min(lo + chunk, rows)
                dz, picked = d_logits(zs[par][j, lo:hi, :], lo, tf_ref[j, 0:1, :], tf_ref[j, 1:2, :], ids)
                ds[par][j, lo:hi, :] = dz
                total = total + picked
            zl_ref[j] = zl_ref[j] + total

        def product(par, j, rows):
            dn_ref[j] += lax.dot_general(
                ds[par][j, 0:rows, :], e_ref[0:rows, :], (((0,), (0,)), ((), ())), preferred_element_type=jnp.float32)

        @pl.when(i == 0)
        def _():
            dn_ref[...] = jnp.zeros_like(dn_ref)
            zl_ref[...] = jnp.zeros_like(zl_ref)
            loop(nb, lambda j: zcopy(0, j, 0, tile).start())
            loop(nb, lambda j: zcopy(1, j, 1, tile).start())

            def first(j):
                zcopy(0, j, 0, tile).wait()
                make(0, 0, j, tile)
                dcopy(0, j, 0, tile).start()

            loop(nb, first)

        def variant(par, next_rows):
            @pl.when(i + 2 < steps - 1)
            def _():
                loop(nb, lambda j: zcopy(par, j, i + 2, tile).start())

            @pl.when(i + 2 == steps - 1)
            def _():
                loop(nb, lambda j: zcopy(par, j, i + 2, last).start())

            def f(j):
                zcopy(1 - par, j, 0, next_rows).wait()

                @pl.when(i >= 1)
                def _():
                    dcopy(1 - par, j, 0, tile).wait()

                product(par, j, tile)
                make(1 - par, i + 1, j, next_rows)
                dcopy(1 - par, j, i + 1, next_rows).start()

            loop(nb, f)

        end = (steps - 1) % 2
        for par in (0, 1):
            @pl.when((i < steps - 2) & (lax.rem(i, 2) == par))
            def _():
                variant(par, tile)

        @pl.when(i == steps - 2)
        def _():
            variant(1 - end, last)

        @pl.when(i == steps - 1)
        def _():
            def f(j):
                product(end, j, last)
                dcopy(end, j, 0, last).wait()
                dcopy(1 - end, j, 0, tile).wait()

            loop(nb, f)

    halves = tokf.shape[0]
    return pl.pallas_call(
        kernel,
        grid_spec=pltpu.PrefetchScalarGridSpec(
            num_scalar_prefetch=1, grid=(steps,),
            in_specs=[full((halves, 8, TB)), full((halves, 1, TB)), pl.BlockSpec((tile, width), lambda i, *_: (i, 0)),
                      any_spec()],
            out_specs=[any_spec(), full((blocks, TB, width)), full((blocks, 8, TB))],
            scratch_shapes=[pltpu.VMEM((blocks, tile, TB), jnp.float32)] * 2
            + [pltpu.VMEM((blocks, tile, TB), jnp.bfloat16)] * 2 + [pltpu.SemaphoreType.DMA((2, blocks))] * 2),
        out_shape=[jax.ShapeDtypeStruct((blocks, vocab, TB), jnp.bfloat16),
                   jax.ShapeDtypeStruct((blocks, TB, width), jnp.float32), jax.ShapeDtypeStruct((blocks, 8, TB), jnp.float32)],
        compiler_params=params(56),
        cost_estimate=pl.CostEstimate(flops=4 * TB * vocab * width, bytes_accessed=100_000_000, transcendentals=0),
        name='pass_two_own',
    )(count, tokf, toki, table, z)


def pass_two_table(own_count, oth_count, tokf, toki, n_own, n_oth, dz_own, z, d_table, after, t0, t1, tile=1280, chunk=64, half=640):
    blocks, _, width = n_own.shape
    vocab = z.shape[1]
    steps = -(-vocab // tile)
    last = vocab - (steps - 1) * tile
    halves = 2 * blocks

    def kernel(own_ref, oth_ref, tf_ref, ti_ref, na_ref, nb_ref, dz_hbm, z_hbm, *rest):
        if d_table is not None:
            rest = rest[2:]
        dt_ref, zl_ref, n_ref, za, zb, da, db, zsem, dsem = rest
        i = pl.program_id(0)
        t = i + t0
        own, oth = own_ref[0], oth_ref[0]
        own_first = lax.axis_index('dp') == 0
        split = jnp.where(own_first, own, oth)
        zs, ds = (za, zb), (da, db)

        def zcopy(par, j, tile_id, rows):
            return pltpu.make_async_copy(
                z_hbm.at[blocks + j, pl.ds(tile_id * tile, rows)], zs[par].at[j, pl.ds(0, rows)], zsem.at[par, j])

        def dcopy(par, j, tile_id, rows):
            return pltpu.make_async_copy(
                dz_hbm.at[j, pl.ds(tile_id * tile, rows)], ds[par].at[j, pl.ds(0, rows)], dsem.at[par, j])

        def load(copy, count, par, tile_id):
            @pl.when((tile_id < t1) & (tile_id < steps - 1))
            def _():
                loop(count, lambda j: copy(par, j, tile_id, tile).start())

            @pl.when((tile_id < t1) & (tile_id == steps - 1))
            def _():
                loop(count, lambda j: copy(par, j, tile_id, last).start())

        def arrive(copy, count, par, tile_id):
            @pl.when((tile_id < t1) & (tile_id < steps - 1))
            def _():
                loop(count, lambda j: copy(par, j, 0, tile).wait())

            @pl.when((tile_id < t1) & (tile_id == steps - 1))
            def _():
                loop(count, lambda j: copy(par, j, 0, last).wait())

        def make(par, tile_id, j, first, end):
            ids = ti_ref[blocks + j, 0:1, :] - tile_id * tile
            total = jnp.zeros((8, TB), jnp.float32)
            for lo in range(first, end, chunk):
                hi = min(lo + chunk, end)
                dz, picked = d_logits(
                    zs[par][j, lo:hi, :], lo, tf_ref[blocks + j, 0:1, :], tf_ref[blocks + j, 1:2, :], ids)
                ds[par][blocks + j, lo:hi, :] = dz
                total = total + picked
            zl_ref[j] = zl_ref[j] + jnp.where(tile_id < t1, total, 0.0)

        def product(par, j, fresh, first, end):
            early = j < split
            local = jnp.where(early, j, j - split)
            block = jnp.where(early == own_first, local, local + blocks)
            part = jnp.dot(ds[par][block, first:end, :], n_ref[block], preferred_element_type=jnp.float32)
            if fresh:
                dt_ref[first:end, :] = part
            else:
                dt_ref[first:end, :] += part

        def mixed(par, j, fresh):
            for first in range(0, tile, half):
                product(par, j, fresh, first, first + half)
                make(1 - par, t + 1, j, first, first + half)

        @pl.when(i == 0)
        def _():
            zl_ref[...] = jnp.zeros_like(zl_ref)
            load(zcopy, oth, 0, t0)
            load(dcopy, own, 0, t0)
            load(zcopy, oth, 1, t0 + 1)
            n_ref[0:blocks] = na_ref[...]
            n_ref[blocks:] = nb_ref[...]
            arrive(zcopy, oth, 0, t0)
            loop(oth, lambda j: make(0, t0, j, 0, tile))

        def variant(par):
            arrive(dcopy, own, par, t)
            arrive(zcopy, oth, 1 - par, t + 1)
            load(zcopy, oth, par, t + 2)
            load(dcopy, own, 1 - par, t + 1)
            mixed(par, 0, True)

            def both(j, _):
                mixed(par, j, False)
                return 0

            def single(j, _):
                product(par, j, False, 0, tile)
                return 0

            lax.fori_loop(1, oth, both, 0)
            lax.fori_loop(oth, own + oth, single, 0)

        for par in (0, 1):
            @pl.when(lax.rem(i, 2) == par)
            def _():
                variant(par)

    operands = [own_count, oth_count, tokf, toki, n_own, n_oth, dz_own, z]
    in_specs = [full((halves, 8, TB)), full((halves, 1, TB)), full((blocks, TB, width)), full((blocks, TB, width)),
                any_spec(), any_spec()]
    aliases = {}
    if d_table is not None:
        operands += [d_table, after]
        in_specs += [any_spec(), any_spec()]
        aliases = {8: 0}
    return pl.pallas_call(
        kernel,
        grid_spec=pltpu.PrefetchScalarGridSpec(
            num_scalar_prefetch=2, grid=(t1 - t0,), in_specs=in_specs,
            out_specs=[pl.BlockSpec((tile, width), lambda i, *_: (i + t0, 0)), full((blocks, 8, TB))],
            scratch_shapes=[pltpu.VMEM((halves, TB, width), jnp.bfloat16)]
            + [pltpu.VMEM((blocks, tile, TB), jnp.float32)] * 2 + [pltpu.VMEM((halves, tile, TB), jnp.bfloat16)] * 2
            + [pltpu.SemaphoreType.DMA((2, blocks))] * 2),
        out_shape=[jax.ShapeDtypeStruct((vocab, width), jnp.float32), jax.ShapeDtypeStruct((blocks, 8, TB), jnp.float32)],
        input_output_aliases=aliases,
        compiler_params=params(52),
        cost_estimate=pl.CostEstimate(
            flops=8 * TB * vocab * width * (t1 - t0) // steps, bytes_accessed=100_000_000, transcendentals=0),
        name='pass_two_table',
    )(*operands)


def all_to_peers(buf, send_sem, recv_sem, peers):
    me, ids = peers
    copies = []
    for r, (target, _) in enumerate(ids):
        copies.append(pltpu.make_async_remote_copy(
            src_ref=buf.at[me], dst_ref=buf.at[me], send_sem=send_sem.at[r], recv_sem=recv_sem.at[r],
            device_id=target, device_id_type=MESH))
    for c in copies:
        c.start()
    return copies


def greet(ids):
    barrier = pltpu.get_barrier_semaphore()
    for target, _ in ids:
        pl.semaphore_signal(barrier, inc=1, device_id=target, device_id_type=MESH)
    pl.semaphore_wait(barrier, len(ids))


def combine_stats(st_own, st_oth, mask_own, mask_oth, vp):
    blocks = st_own.shape[0]
    rows = 2 * blocks

    def kernel(a_ref, b_ref, ma_ref, mb_ref, tf_ref, sum_ref, buf, send_sem, recv_sem):
        me = lax.axis_index('vp')
        dp = lax.axis_index('dp')
        ids = [((dp, lax.rem(me + r, vp)), None) for r in range(1, vp)]
        buf[me] = jnp.zeros((16, TB), jnp.float32)
        for k in range(rows):
            st = (a_ref if k < blocks else b_ref)[k % blocks]
            top = jnp.max(st[0:8], axis=0, keepdims=True)
            total = jnp.sum(st[8:16] * jnp.exp2(st[0:8] - top), axis=0, keepdims=True)
            buf[me, k:k + 1, :] = top
            buf[me, 8 + k:9 + k, :] = total
        greet(ids)
        for c in all_to_peers(buf, send_sem, recv_sem, (me, ids)):
            c.wait()
        top = buf[0, 0:8, :]
        for k in range(1, vp):
            top = jnp.maximum(top, buf[k, 0:8, :])
        total = jnp.zeros_like(top)
        for k in range(vp):
            total = total + buf[k, 8:16, :] * jnp.exp2(buf[k, 0:8, :] - top)
        masks = jnp.concatenate([ma_ref[...], mb_ref[...], jnp.zeros((8 - rows, TB), jnp.float32)], axis=0)
        log_norm = top + jnp.log2(total)
        count = jnp.sum(masks)
        weight = masks * (LOGIT_SCALE / count)
        shift = log_norm - jnp.log2(weight)
        for k in range(rows):
            tf_ref[k] = jnp.concatenate(
                [shift[k:k + 1], weight[k:k + 1], jnp.zeros((6, TB), jnp.float32)], axis=0)
        kept = jnp.where(masks > 0.0, log_norm * LN2, 0.0)
        both = jnp.sum(kept[0:blocks]) + jnp.sum(kept[blocks:rows])
        sum_ref[...] = jnp.full((8, 128), both / count, jnp.float32)

    return pl.pallas_call(
        kernel,
        out_shape=[jax.ShapeDtypeStruct((rows, 8, TB), jnp.float32), jax.ShapeDtypeStruct((8, 128), jnp.float32)],
        in_specs=[pl.BlockSpec(memory_space=pltpu.VMEM)] * 4,
        out_specs=[pl.BlockSpec(memory_space=pltpu.VMEM)] * 2,
        scratch_shapes=[pltpu.VMEM((vp, 16, TB), jnp.float32), pltpu.SemaphoreType.DMA((vp - 1,)),
                        pltpu.SemaphoreType.DMA((vp - 1,))],
        compiler_params=pltpu.CompilerParams(collective_id=0, has_side_effects=True),
        name='combine_stats',
    )(st_own, st_oth, mask_own, mask_oth)


def norm_back(d_normed, compact, gain, after):
    tokens, width = d_normed.shape

    def kernel(dn_ref, h_ref, g_ref, _, dh_ref, dg_ref):
        dn = dn_ref[...]
        x_hat, inv_std = normalise(h_ref[...])
        scaled = dn * g_ref[...]
        mean_one = jnp.mean(scaled, axis=-1, keepdims=True)
        mean_two = jnp.mean(scaled * x_hat, axis=-1, keepdims=True)
        grad = (inv_std * (scaled - mean_one - x_hat * mean_two)).astype(jnp.bfloat16)
        dh_ref[...] = grad.astype(jnp.float32)
        dg_ref[...] = jnp.sum((dn * x_hat).reshape(tokens // 8, 8, width), axis=0)

    return pl.pallas_call(
        kernel,
        out_shape=[jax.ShapeDtypeStruct((tokens, width), jnp.float32), jax.ShapeDtypeStruct((8, width), jnp.float32)],
        in_specs=[pl.BlockSpec(memory_space=pltpu.VMEM)] * 3 + [any_spec()],
        name='norm_back',
    )(d_normed, compact, gain, after)


def finish(grads, mask, partial, picked, masks, lse_sum, dp_size, vp):
    tokens, width = grads.shape
    group = dp_size * vp
    gain_rows = width // 128
    rows = gain_rows + 8

    def kernel(g_ref, t_ref, p_ref, z_ref, m_ref, s_ref, dh_ref, dg_ref, loss_ref, buf, held, send_sem, recv_sem, copy_sem):
        fetch = pltpu.make_async_copy(g_ref, held, copy_sem)
        fetch.start()
        me = lax.axis_index('dp') * vp + lax.axis_index('vp')
        ids = []
        for r in range(1, group):
            other = lax.rem(me + r, group)
            ids.append(((lax.div(other, vp), lax.rem(other, vp)), None))
        total = jnp.sum(p_ref[...], axis=0, keepdims=True)
        for k in range(gain_rows):
            buf[me, k:k + 1, :] = total[:, k * 128:(k + 1) * 128]
        masks = m_ref[...]
        kept = jnp.where(masks > 0.0, jnp.sum(z_ref[...], axis=1), 0.0)
        half = kept.shape[0] // 2
        both = jnp.sum(kept[:half]) + jnp.sum(kept[half:])
        buf[me, gain_rows:, :] = jnp.full((8, 128), both * LN2 / jnp.sum(masks), jnp.float32)
        greet(ids)
        copies = all_to_peers(buf, send_sem, recv_sem, (me, ids))
        sel = selection(one_row(t_ref))
        fetch.wait()
        dh_ref[...] = lax.dot_general(
            sel, held[...].astype(jnp.bfloat16), (((0,), (0,)), ((), ())), preferred_element_type=jnp.float32).astype(jnp.bfloat16)
        for c in copies:
            c.wait()
        total = buf[0]
        for k in range(1, group):
            total = total + buf[k]
        dg_ref[...] = total[:gain_rows]
        loss_ref[...] = s_ref[...] - total[gain_rows:] * (1.0 / dp_size)

    return pl.pallas_call(
        kernel,
        out_shape=[jax.ShapeDtypeStruct((tokens, width), jnp.bfloat16), jax.ShapeDtypeStruct((gain_rows, 128), jnp.float32),
                   jax.ShapeDtypeStruct((8, 128), jnp.float32)],
        in_specs=[pl.BlockSpec(memory_space=pltpu.HBM)] + [pl.BlockSpec(memory_space=pltpu.VMEM)] * 5,
        out_specs=[pl.BlockSpec(memory_space=pltpu.VMEM)] * 3,
        scratch_shapes=[pltpu.VMEM((group, rows, 128), jnp.float32), pltpu.VMEM((tokens, width), jnp.float32),
                        pltpu.SemaphoreType.DMA((group - 1,)), pltpu.SemaphoreType.DMA((group - 1,)), pltpu.SemaphoreType.DMA],
        compiler_params=params(48, collective_id=1, has_side_effects=True),
        name='finish',
    )(grads, mask, partial, picked, masks, lse_sum)


def solution(mesh):
    dp_size, vp = mesh.shape['dp'], mesh.shape['vp']

    def local_step(hidden, norm_gain, emb_table, labels, tok_mask):
        rows, seq_len, width = hidden.shape
        vocab = emb_table.shape[0]
        tokens = rows * seq_len
        blocks = tokens // TB
        share = tokens // vp
        my_vp = lax.axis_index('vp')
        my_dp = lax.axis_index('dp')
        gain = norm_gain.reshape(1, width)
        n_own, piece, compact, meta, nb_own = prologue(
            hidden.reshape(tokens, width), gain, labels, tok_mask, vp)
        pieces = lax.all_gather(piece, ('dp', 'vp'), axis=0)
        z, st_own = pass_one(nb_own, jnp.zeros((1,), jnp.int32), n_own, emb_table, None, 0, blocks)
        meta_oth = lax.dynamic_slice(pieces, ((1 - my_dp) * vp, share, 0), (1, 2, tokens))[0]
        nb_oth = lax.div(jnp.sum(meta_oth[1]).astype(jnp.int32) + (TB - 1), TB)[None]
        z, st_oth, n_oth = pass_one(nb_oth, (1 - my_dp)[None], pieces, emb_table, z, blocks, blocks)
        n_own, n_oth = n_own.reshape(blocks, TB, width), n_oth.reshape(blocks, TB, width)
        mask_own, mask_oth = meta[1].reshape(blocks, TB), meta_oth[1].reshape(blocks, TB)
        tokf, lse_sum = combine_stats(st_own, st_oth, mask_own, mask_oth, vp)
        ids = jnp.concatenate([meta[0], meta_oth[0]]).astype(jnp.int32).reshape(2 * blocks, 1, TB) - my_vp * vocab
        toki = jnp.where((ids >= 0) & (ids < vocab), ids, -vocab)
        dz_own, d_part, picked = pass_two_own(nb_own, tokf, toki, emb_table, z, blocks)
        d_share = lax.psum_scatter(d_part.reshape(tokens, width), 'vp', scatter_dimension=0, tiled=True)
        args = (nb_own, nb_oth, tokf, toki, n_own, n_oth, dz_own, z)
        steps, cut = -(-vocab // 1280), SPLIT
        d_table, picked_a = pass_two_table(*args, None, None, 0, cut)
        grads, gain_part = norm_back(d_share, compact, gain, picked_a)
        d_table, picked_b = pass_two_table(*args, d_table, gain_part, cut, steps)
        all_grads = lax.all_gather(grads, 'vp', axis=0, tiled=True)
        d_hidden, d_gain, loss = finish(
            all_grads, tok_mask, gain_part, jnp.concatenate([picked, picked_a + picked_b]),
            jnp.concatenate([mask_own, mask_oth]), lse_sum, dp_size, vp)
        return loss[0, 0], d_table, d_hidden.reshape(rows, seq_len, width), d_gain.reshape(width)

    return jax.shard_map(
        local_step, mesh=mesh,
        in_specs=(P('dp', None, None), P(None), P('vp', None), P('dp', None), P('dp', None)),
        out_specs=(P(), P('vp', None), P('dp', None, None), P(None)), check_vma=False)
```

```python
import functools

import jax
import jax.numpy as jnp
from jax import lax
from jax.experimental import pallas as pl
from jax.experimental.pallas import tpu as pltpu
from jax.sharding import PartitionSpec as P

LOGIT_SCALE = 0.0625
EPS = 1e-5
LOG2E = 1.4426950408889634
LN2 = 0.6931471805599453
C2 = LOGIT_SCALE * LOG2E
TB = 256
SPLIT = 9
MIB = 1024 * 1024
NEG = -3e38
MESH = pl.DeviceIdType.MESH


def full(shape):
    return pl.BlockSpec(shape, lambda *_: (0,) * len(shape))


def any_spec():
    return pl.BlockSpec(memory_space=pl.ANY)


def params(limit, **kw):
    return pltpu.CompilerParams(vmem_limit_bytes=limit * MIB, **kw)


def selection(mask_row):
    tokens = mask_row.shape[1]
    rows = lax.broadcasted_iota(jnp.int32, (tokens, tokens), 0)
    cols = lax.broadcasted_iota(jnp.int32, (tokens, tokens), 1)
    upper = jnp.where(rows <= cols, 1.0, 0.0).astype(jnp.bfloat16)
    lhs = jnp.broadcast_to(mask_row, (8, tokens)).astype(jnp.bfloat16)
    rank = jnp.dot(lhs, upper, preferred_element_type=jnp.float32)[0:1]
    hit = (rows.astype(jnp.float32) == rank - 1.0) & (mask_row > 0.0)
    return jnp.where(hit, 1.0, 0.0).astype(jnp.bfloat16)


def one_row(ref):
    return jnp.concatenate([ref[r:r + 1, :] for r in range(ref.shape[0])], axis=1)


def normalise(values):
    mean_x = jnp.mean(values, axis=-1, keepdims=True)
    centered = values - mean_x
    variance = jnp.mean(centered * centered, axis=-1, keepdims=True)
    inv_std = lax.rsqrt(variance + EPS)
    return centered * inv_std, inv_std


def prologue(hidden, gain, labels, mask, vp):
    tokens, width = hidden.shape
    share = tokens // vp

    def kernel(h_hbm, g_hbm, l_hbm, m_hbm, n_ref, piece_ref, hc_ref, meta_ref, nb_ref, wide_ref, h_ref, g_ref, l_ref, m_ref,
               sem):
        pairs = ((h_hbm, h_ref), (g_hbm, g_ref), (l_hbm, l_ref), (m_hbm, m_ref))
        copies = [pltpu.make_async_copy(src, dst, sem.at[k]) for k, (src, dst) in enumerate(pairs)]
        for c in copies:
            c.start()
        for c in copies:
            c.wait()
        mask_row = one_row(m_ref)
        sel = selection(mask_row)
        compact = jnp.dot(sel, h_ref[...], preferred_element_type=jnp.float32)
        mine = pl.multiple_of(lax.axis_index('vp') * share, share)
        wide_ref[0] = compact
        hc_ref[...] = wide_ref[0, pl.ds(mine, share), :]
        x_hat, _ = normalise(compact)
        normed = (g_ref[...] * x_hat).astype(jnp.bfloat16)
        n_ref[...] = normed
        wide_ref[1] = normed.astype(jnp.float32)
        piece_ref[0:share, :] = wide_ref[1, pl.ds(mine, share), :]
        ids = one_row(l_ref)
        high, mid, low = ids >> 16, (ids >> 8) & 255, ids & 255
        pieces = [p.astype(jnp.float32) for p in (high, mid, low)] + [mask_row]
        stack = jnp.concatenate(pieces + [jnp.zeros((4, tokens), jnp.float32)], axis=0).astype(jnp.bfloat16)
        moved = lax.dot_general(stack, sel, (((1,), (1,)), ((), ())), preferred_element_type=jnp.float32)
        label_row = moved[0:1] * 65536.0 + moved[1:2] * 256.0 + moved[2:3]
        meta = jnp.concatenate([label_row, moved[3:4], jnp.zeros((6, tokens), jnp.float32)], axis=0)
        meta_ref[...] = meta
        piece_ref[share:share + 8, 0:tokens] = meta
        piece_ref[share:share + 8, tokens:] = jnp.zeros((8, width - tokens), jnp.float32)
        nb_ref[0] = lax.div(jnp.sum(mask_row).astype(jnp.int32) + (TB - 1), TB)

    return pl.pallas_call(
        kernel,
        out_shape=[
            jax.ShapeDtypeStruct((tokens, width), jnp.bfloat16),
            jax.ShapeDtypeStruct((share + 8, width), jnp.float32),
            jax.ShapeDtypeStruct((share, width), jnp.float32),
            jax.ShapeDtypeStruct((8, tokens), jnp.float32),
            jax.ShapeDtypeStruct((1,), jnp.int32),
        ],
        out_specs=[pl.BlockSpec(memory_space=pltpu.VMEM)] * 4 + [pl.BlockSpec(memory_space=pltpu.SMEM)],
        in_specs=[pl.BlockSpec(memory_space=pltpu.HBM)] * 4,
        scratch_shapes=[pltpu.VMEM((2, tokens, width), jnp.float32)]
        + [pltpu.VMEM(a.shape, a.dtype) for a in (hidden, gain, labels, mask)] + [pltpu.SemaphoreType.DMA((4,))],
        compiler_params=params(63),
        cost_estimate=pl.CostEstimate(flops=3_000_000_000, bytes_accessed=8_000_000, transcendentals=0),
        name='prologue',
    )(hidden, gain, labels, mask)


def pass_one(count, part, normed, table, z_in, first_block, blocks, tile=2560, slots=6, chunk=64):
    total_blocks = 2 * blocks
    vocab, width = table.shape
    steps = -(-vocab // tile)
    last = vocab - (steps - 1) * tile
    cast = normed.dtype != jnp.bfloat16
    tokens = blocks * TB
    share = normed.shape[1] - 8
    groups = tokens // share if cast else 1

    def kernel(nb_ref, _, n_ref, e_ref, *rest):
        if z_in is not None:
            rest = rest[1:]
        if cast:
            z_hbm, st_ref, nout_ref, zbuf, sem = rest
        else:
            z_hbm, st_ref, zbuf, sem = rest
            nout_ref = n_ref
        i = pl.program_id(0)
        nb = nb_ref[0]

        @pl.when(i == 0)
        def _():
            st_ref[:, 0:8, :] = jnp.full((blocks, 8, TB), NEG, jnp.float32)
            st_ref[:, 8:16, :] = jnp.zeros((blocks, 8, TB), jnp.float32)
            if cast:
                for k in range(groups):
                    nout_ref[k * share:(k + 1) * share, :] = n_ref[k, 0:share, :].astype(jnp.bfloat16)

        def copy(block, slot, rows, base=0):
            return pltpu.make_async_copy(
                zbuf.at[slot, pl.ds(0, rows)], z_hbm.at[first_block + block, pl.ds(base, rows)], sem.at[slot])

        def body(rows):
            def step(j, _):
                g = i * nb + j
                slot = lax.rem(g, slots)

                @pl.when(g >= slots)
                def _():
                    copy(0, slot, tile).wait()

                run_max = st_ref[j, 0:8, :]
                run_sum = st_ref[j, 8:16, :]
                block = nout_ref[pl.ds(pl.multiple_of(j * TB, TB), TB), :]
                zbuf[slot, 0:rows, :] = C2 * lax.dot_general(
                    e_ref[0:rows], block, (((1,), (1,)), ((), ())), preferred_element_type=jnp.float32)
                for lo in range(0, rows, chunk):
                    hi = min(lo + chunk, rows)
                    parts = zbuf[slot, lo:hi, :].reshape((hi - lo) // 8, 8, TB)
                    new_max = jnp.maximum(run_max, jnp.max(parts, axis=0))
                    total = jnp.sum(jnp.exp2(parts - new_max[None]), axis=0)
                    run_sum = run_sum * jnp.exp2(run_max - new_max) + total
                    run_max = new_max
                st_ref[j, 0:8, :] = run_max
                st_ref[j, 8:16, :] = run_sum
                copy(j, slot, rows, i * tile).start()
                return 0

            lax.fori_loop(0, nb, step, 0)

        @pl.when(i < steps - 1)
        def _():
            body(tile)

        @pl.when(i == steps - 1)
        def _():
            body(last)
            end = steps * nb
            for q in range(slots):
                slot = lax.rem(end - 1 - q + slots, slots)

                @pl.when(q < nb)
                def _():
                    copy(0, slot, last).wait()

                @pl.when((q >= nb) & (end - 1 - q >= 0))
                def _():
                    copy(0, slot, tile).wait()

    out_shape = [
        jax.ShapeDtypeStruct((total_blocks, vocab, TB), jnp.float32),
        jax.ShapeDtypeStruct((blocks, 16, TB), jnp.float32),
    ]
    out_specs = [any_spec(), full((blocks, 16, TB))]
    if cast:
        out_shape.append(jax.ShapeDtypeStruct((tokens, width), jnp.bfloat16))
        out_specs.append(full((tokens, width)))
        n_spec = pl.BlockSpec((groups, share + 8, width), lambda i, nb, part: (part[0], 0, 0))
    else:
        n_spec = full((tokens, width))
    operands = [count, part, normed, table]
    in_specs = [n_spec, pl.BlockSpec((tile, width), lambda i, *_: (i, 0))]
    aliases = {}
    if z_in is not None:
        operands.append(z_in)
        in_specs.append(any_spec())
        aliases = {4: 0}
    return pl.pallas_call(
        kernel,
        grid_spec=pltpu.PrefetchScalarGridSpec(
            num_scalar_prefetch=2, grid=(steps,), in_specs=in_specs, out_specs=out_specs,
            scratch_shapes=[pltpu.VMEM((slots, tile, TB), jnp.float32), pltpu.SemaphoreType.DMA((slots,))]),
        out_shape=out_shape,
        input_output_aliases=aliases,
        compiler_params=params(50),
        cost_estimate=pl.CostEstimate(flops=2 * 2 * TB * vocab * width, bytes_accessed=80_000_000, transcendentals=0),
        name='pass_one',
    )(*operands)


def d_logits(zc, lo, shift, weight, ids):
    scaled = jnp.exp2(zc - shift)
    hit = lax.broadcasted_iota(jnp.int32, zc.shape, 0) == (ids - lo)
    dz = jnp.where(hit, scaled - weight, scaled).astype(jnp.bfloat16)
    picked = jnp.where(hit, zc, 0.0)
    return dz, jnp.sum(picked.reshape(zc.shape[0] // 8, 8, zc.shape[1]), axis=0)


def loop(count, f):
    lax.fori_loop(0, count, lambda j, _: (f(j), 0)[1], 0)


def pass_two_own(count, tokf, toki, table, z, blocks, tile=1280, chunk=32):
    vocab, width = table.shape
    steps = -(-vocab // tile)
    last = vocab - (steps - 1) * tile

    def kernel(nb_ref, tf_ref, ti_ref, e_ref, z_hbm, dz_hbm, dn_ref, zl_ref, za, zb, da, db, zsem, dsem):
        i = pl.program_id(0)
        nb = nb_ref[0]
        zs, ds = (za, zb), (da, db)

        def zcopy(par, j, t, rows):
            return pltpu.make_async_copy(
                z_hbm.at[j, pl.ds(t * tile, rows)], zs[par].at[j, pl.ds(0, rows)], zsem.at[par, j])

        def dcopy(par, j, t, rows):
            return pltpu.make_async_copy(
                ds[par].at[j, pl.ds(0, rows)], dz_hbm.at[j, pl.ds(t * tile, rows)], dsem.at[par, j])

        def make(par, t, j, rows):
            ids = ti_ref[j, 0:1, :] - t * tile
            total = jnp.zeros((8, TB), jnp.float32)
            for lo in range(0, rows, chunk):
                hi = min(lo + chunk, rows)
                dz, picked = d_logits(zs[par][j, lo:hi, :], lo, tf_ref[j, 0:1, :], tf_ref[j, 1:2, :], ids)
                ds[par][j, lo:hi, :] = dz
                total = total + picked
            zl_ref[j] = zl_ref[j] + total

        def product(par, j, rows):
            dn_ref[j] += lax.dot_general(
                ds[par][j, 0:rows, :], e_ref[0:rows, :], (((0,), (0,)), ((), ())), preferred_element_type=jnp.float32)

        @pl.when(i == 0)
        def _():
            dn_ref[...] = jnp.zeros_like(dn_ref)
            zl_ref[...] = jnp.zeros_like(zl_ref)
            loop(nb, lambda j: zcopy(0, j, 0, tile).start())
            loop(nb, lambda j: zcopy(1, j, 1, tile).start())

            def first(j):
                zcopy(0, j, 0, tile).wait()
                make(0, 0, j, tile)
                dcopy(0, j, 0, tile).start()

            loop(nb, first)

        def variant(par, next_rows):
            @pl.when(i + 2 < steps - 1)
            def _():
                loop(nb, lambda j: zcopy(par, j, i + 2, tile).start())

            @pl.when(i + 2 == steps - 1)
            def _():
                loop(nb, lambda j: zcopy(par, j, i + 2, last).start())

            def f(j):
                zcopy(1 - par, j, 0, next_rows).wait()

                @pl.when(i >= 1)
                def _():
                    dcopy(1 - par, j, 0, tile).wait()

                product(par, j, tile)
                make(1 - par, i + 1, j, next_rows)
                dcopy(1 - par, j, i + 1, next_rows).start()

            loop(nb, f)

        end = (steps - 1) % 2
        for par in (0, 1):
            @pl.when((i < steps - 2) & (lax.rem(i, 2) == par))
            def _():
                variant(par, tile)

        @pl.when(i == steps - 2)
        def _():
            variant(1 - end, last)

        @pl.when(i == steps - 1)
        def _():
            def f(j):
                product(end, j, last)
                dcopy(end, j, 0, last).wait()
                dcopy(1 - end, j, 0, tile).wait()

            loop(nb, f)

    halves = tokf.shape[0]
    return pl.pallas_call(
        kernel,
        grid_spec=pltpu.PrefetchScalarGridSpec(
            num_scalar_prefetch=1, grid=(steps,),
            in_specs=[full((halves, 8, TB)), full((halves, 1, TB)), pl.BlockSpec((tile, width), lambda i, *_: (i, 0)),
                      any_spec()],
            out_specs=[any_spec(), full((blocks, TB, width)), full((blocks, 8, TB))],
            scratch_shapes=[pltpu.VMEM((blocks, tile, TB), jnp.float32)] * 2
            + [pltpu.VMEM((blocks, tile, TB), jnp.bfloat16)] * 2 + [pltpu.SemaphoreType.DMA((2, blocks))] * 2),
        out_shape=[jax.ShapeDtypeStruct((blocks, vocab, TB), jnp.bfloat16),
                   jax.ShapeDtypeStruct((blocks, TB, width), jnp.float32), jax.ShapeDtypeStruct((blocks, 8, TB), jnp.float32)],
        compiler_params=params(56),
        cost_estimate=pl.CostEstimate(flops=4 * TB * vocab * width, bytes_accessed=100_000_000, transcendentals=0),
        name='pass_two_own',
    )(count, tokf, toki, table, z)


def pass_two_table(own_count, oth_count, tokf, toki, n_own, n_oth, dz_own, z, d_table, after, t0, t1, tile=1280, chunk=64, half=640):
    blocks, _, width = n_own.shape
    vocab = z.shape[1]
    steps = -(-vocab // tile)
    last = vocab - (steps - 1) * tile
    halves = 2 * blocks

    def kernel(own_ref, oth_ref, tf_ref, ti_ref, na_ref, nb_ref, dz_hbm, z_hbm, *rest):
        if d_table is not None:
            rest = rest[2:]
        dt_ref, zl_ref, n_ref, za, zb, da, db, zsem, dsem = rest
        i = pl.program_id(0)
        t = i + t0
        own, oth = own_ref[0], oth_ref[0]
        own_first = lax.axis_index('dp') == 0
        split = jnp.where(own_first, own, oth)
        zs, ds = (za, zb), (da, db)

        def zcopy(par, j, tile_id, rows):
            return pltpu.make_async_copy(
                z_hbm.at[blocks + j, pl.ds(tile_id * tile, rows)], zs[par].at[j, pl.ds(0, rows)], zsem.at[par, j])

        def dcopy(par, j, tile_id, rows):
            return pltpu.make_async_copy(
                dz_hbm.at[j, pl.ds(tile_id * tile, rows)], ds[par].at[j, pl.ds(0, rows)], dsem.at[par, j])

        def load(copy, count, par, tile_id):
            @pl.when((tile_id < t1) & (tile_id < steps - 1))
            def _():
                loop(count, lambda j: copy(par, j, tile_id, tile).start())

            @pl.when((tile_id < t1) & (tile_id == steps - 1))
            def _():
                loop(count, lambda j: copy(par, j, tile_id, last).start())

        def arrive(copy, count, par, tile_id):
            @pl.when((tile_id < t1) & (tile_id < steps - 1))
            def _():
                loop(count, lambda j: copy(par, j, 0, tile).wait())

            @pl.when((tile_id < t1) & (tile_id == steps - 1))
            def _():
                loop(count, lambda j: copy(par, j, 0, last).wait())

        def make(par, tile_id, j, first, end):
            ids = ti_ref[blocks + j, 0:1, :] - tile_id * tile
            total = jnp.zeros((8, TB), jnp.float32)
            for lo in range(first, end, chunk):
                hi = min(lo + chunk, end)
                dz, picked = d_logits(
                    zs[par][j, lo:hi, :], lo, tf_ref[blocks + j, 0:1, :], tf_ref[blocks + j, 1:2, :], ids)
                ds[par][blocks + j, lo:hi, :] = dz
                total = total + picked
            zl_ref[j] = zl_ref[j] + jnp.where(tile_id < t1, total, 0.0)

        def product(par, j, fresh, first, end):
            early = j < split
            local = jnp.where(early, j, j - split)
            block = jnp.where(early == own_first, local, local + blocks)
            part = jnp.dot(ds[par][block, first:end, :], n_ref[block], preferred_element_type=jnp.float32)
            if fresh:
                dt_ref[first:end, :] = part
            else:
                dt_ref[first:end, :] += part

        def mixed(par, j, fresh):
            for first in range(0, tile, half):
                product(par, j, fresh, first, first + half)
                make(1 - par, t + 1, j, first, first + half)

        @pl.when(i == 0)
        def _():
            zl_ref[...] = jnp.zeros_like(zl_ref)
            load(zcopy, oth, 0, t0)
            load(dcopy, own, 0, t0)
            load(zcopy, oth, 1, t0 + 1)
            n_ref[0:blocks] = na_ref[...]
            n_ref[blocks:] = nb_ref[...]
            arrive(zcopy, oth, 0, t0)
            loop(oth, lambda j: make(0, t0, j, 0, tile))

        def variant(par):
            arrive(dcopy, own, par, t)
            arrive(zcopy, oth, 1 - par, t + 1)
            load(zcopy, oth, par, t + 2)
            load(dcopy, own, 1 - par, t + 1)
            mixed(par, 0, True)

            def both(j, _):
                mixed(par, j, False)
                return 0

            def single(j, _):
                product(par, j, False, 0, tile)
                return 0

            lax.fori_loop(1, oth, both, 0)
            lax.fori_loop(oth, own + oth, single, 0)

        for par in (0, 1):
            @pl.when(lax.rem(i, 2) == par)
            def _():
                variant(par)

    operands = [own_count, oth_count, tokf, toki, n_own, n_oth, dz_own, z]
    in_specs = [full((halves, 8, TB)), full((halves, 1, TB)), full((blocks, TB, width)), full((blocks, TB, width)),
                any_spec(), any_spec()]
    aliases = {}
    if d_table is not None:
        operands += [d_table, after]
        in_specs += [any_spec(), any_spec()]
        aliases = {8: 0}
    return pl.pallas_call(
        kernel,
        grid_spec=pltpu.PrefetchScalarGridSpec(
            num_scalar_prefetch=2, grid=(t1 - t0,), in_specs=in_specs,
            out_specs=[pl.BlockSpec((tile, width), lambda i, *_: (i + t0, 0)), full((blocks, 8, TB))],
            scratch_shapes=[pltpu.VMEM((halves, TB, width), jnp.bfloat16)]
            + [pltpu.VMEM((blocks, tile, TB), jnp.float32)] * 2 + [pltpu.VMEM((halves, tile, TB), jnp.bfloat16)] * 2
            + [pltpu.SemaphoreType.DMA((2, blocks))] * 2),
        out_shape=[jax.ShapeDtypeStruct((vocab, width), jnp.float32), jax.ShapeDtypeStruct((blocks, 8, TB), jnp.float32)],
        input_output_aliases=aliases,
        compiler_params=params(52),
        cost_estimate=pl.CostEstimate(
            flops=8 * TB * vocab * width * (t1 - t0) // steps, bytes_accessed=100_000_000, transcendentals=0),
        name='pass_two_table',
    )(*operands)


def all_to_peers(buf, send_sem, recv_sem, peers):
    me, ids = peers
    copies = []
    for r, (target, _) in enumerate(ids):
        copies.append(pltpu.make_async_remote_copy(
            src_ref=buf.at[me], dst_ref=buf.at[me], send_sem=send_sem.at[r], recv_sem=recv_sem.at[r],
            device_id=target, device_id_type=MESH))
    for c in copies:
        c.start()
    return copies


def greet(ids):
    barrier = pltpu.get_barrier_semaphore()
    for target, _ in ids:
        pl.semaphore_signal(barrier, inc=1, device_id=target, device_id_type=MESH)
    pl.semaphore_wait(barrier, len(ids))


def combine_stats(st_own, st_oth, mask_own, mask_oth, vp):
    blocks = st_own.shape[0]
    rows = 2 * blocks

    def kernel(a_ref, b_ref, ma_ref, mb_ref, tf_ref, sum_ref, buf, send_sem, recv_sem):
        me = lax.axis_index('vp')
        dp = lax.axis_index('dp')
        ids = [((dp, lax.rem(me + r, vp)), None) for r in range(1, vp)]
        buf[me] = jnp.zeros((16, TB), jnp.float32)
        for k in range(rows):
            st = (a_ref if k < blocks else b_ref)[k % blocks]
            top = jnp.max(st[0:8], axis=0, keepdims=True)
            total = jnp.sum(st[8:16] * jnp.exp2(st[0:8] - top), axis=0, keepdims=True)
            buf[me, k:k + 1, :] = top
            buf[me, 8 + k:9 + k, :] = total
        greet(ids)
        for c in all_to_peers(buf, send_sem, recv_sem, (me, ids)):
            c.wait()
        top = buf[0, 0:8, :]
        for k in range(1, vp):
            top = jnp.maximum(top, buf[k, 0:8, :])
        total = jnp.zeros_like(top)
        for k in range(vp):
            total = total + buf[k, 8:16, :] * jnp.exp2(buf[k, 0:8, :] - top)
        masks = jnp.concatenate([ma_ref[...], mb_ref[...], jnp.zeros((8 - rows, TB), jnp.float32)], axis=0)
        log_norm = top + jnp.log2(total)
        count = jnp.sum(masks)
        weight = masks * (LOGIT_SCALE / count)
        shift = log_norm - jnp.log2(weight)
        for k in range(rows):
            tf_ref[k] = jnp.concatenate(
                [shift[k:k + 1], weight[k:k + 1], jnp.zeros((6, TB), jnp.float32)], axis=0)
        kept = jnp.where(masks > 0.0, log_norm * LN2, 0.0)
        both = jnp.sum(kept[0:blocks]) + jnp.sum(kept[blocks:rows])
        sum_ref[...] = jnp.full((8, 128), both / count, jnp.float32)

    return pl.pallas_call(
        kernel,
        out_shape=[jax.ShapeDtypeStruct((rows, 8, TB), jnp.float32), jax.ShapeDtypeStruct((8, 128), jnp.float32)],
        in_specs=[pl.BlockSpec(memory_space=pltpu.VMEM)] * 4,
        out_specs=[pl.BlockSpec(memory_space=pltpu.VMEM)] * 2,
        scratch_shapes=[pltpu.VMEM((vp, 16, TB), jnp.float32), pltpu.SemaphoreType.DMA((vp - 1,)),
                        pltpu.SemaphoreType.DMA((vp - 1,))],
        compiler_params=pltpu.CompilerParams(collective_id=0, has_side_effects=True),
        name='combine_stats',
    )(st_own, st_oth, mask_own, mask_oth)


def norm_back(d_normed, compact, gain, after):
    tokens, width = d_normed.shape

    def kernel(dn_ref, h_ref, g_ref, _, dh_ref, dg_ref):
        dn = dn_ref[...]
        x_hat, inv_std = normalise(h_ref[...])
        scaled = dn * g_ref[...]
        mean_one = jnp.mean(scaled, axis=-1, keepdims=True)
        mean_two = jnp.mean(scaled * x_hat, axis=-1, keepdims=True)
        grad = (inv_std * (scaled - mean_one - x_hat * mean_two)).astype(jnp.bfloat16)
        dh_ref[...] = grad.astype(jnp.float32)
        dg_ref[...] = jnp.sum((dn * x_hat).reshape(tokens // 8, 8, width), axis=0)

    return pl.pallas_call(
        kernel,
        out_shape=[jax.ShapeDtypeStruct((tokens, width), jnp.float32), jax.ShapeDtypeStruct((8, width), jnp.float32)],
        in_specs=[pl.BlockSpec(memory_space=pltpu.VMEM)] * 3 + [any_spec()],
        name='norm_back',
    )(d_normed, compact, gain, after)


def finish(grads, mask, partial, picked, masks, lse_sum, dp_size, vp):
    tokens, width = grads.shape
    group = dp_size * vp
    gain_rows = width // 128
    rows = gain_rows + 8

    def kernel(g_ref, t_ref, p_ref, z_ref, m_ref, s_ref, dh_ref, dg_ref, loss_ref, buf, held, send_sem, recv_sem, copy_sem):
        fetch = pltpu.make_async_copy(g_ref, held, copy_sem)
        fetch.start()
        me = lax.axis_index('dp') * vp + lax.axis_index('vp')
        ids = []
        for r in range(1, group):
            other = lax.rem(me + r, group)
            ids.append(((lax.div(other, vp), lax.rem(other, vp)), None))
        total = jnp.sum(p_ref[...], axis=0, keepdims=True)
        for k in range(gain_rows):
            buf[me, k:k + 1, :] = total[:, k * 128:(k + 1) * 128]
        masks = m_ref[...]
        kept = jnp.where(masks > 0.0, jnp.sum(z_ref[...], axis=1), 0.0)
        half = kept.shape[0] // 2
        both = jnp.sum(kept[:half]) + jnp.sum(kept[half:])
        buf[me, gain_rows:, :] = jnp.full((8, 128), both * LN2 / jnp.sum(masks), jnp.float32)
        greet(ids)
        copies = all_to_peers(buf, send_sem, recv_sem, (me, ids))
        sel = selection(one_row(t_ref))
        fetch.wait()
        dh_ref[...] = lax.dot_general(
            sel, held[...].astype(jnp.bfloat16), (((0,), (0,)), ((), ())), preferred_element_type=jnp.float32).astype(jnp.bfloat16)
        for c in copies:
            c.wait()
        total = buf[0]
        for k in range(1, group):
            total = total + buf[k]
        dg_ref[...] = total[:gain_rows]
        loss_ref[...] = s_ref[...] - total[gain_rows:] * (1.0 / dp_size)

    return pl.pallas_call(
        kernel,
        out_shape=[jax.ShapeDtypeStruct((tokens, width), jnp.bfloat16), jax.ShapeDtypeStruct((gain_rows, 128), jnp.float32),
                   jax.ShapeDtypeStruct((8, 128), jnp.float32)],
        in_specs=[pl.BlockSpec(memory_space=pltpu.HBM)] + [pl.BlockSpec(memory_space=pltpu.VMEM)] * 5,
        out_specs=[pl.BlockSpec(memory_space=pltpu.VMEM)] * 3,
        scratch_shapes=[pltpu.VMEM((group, rows, 128), jnp.float32), pltpu.VMEM((tokens, width), jnp.float32),
                        pltpu.SemaphoreType.DMA((group - 1,)), pltpu.SemaphoreType.DMA((group - 1,)), pltpu.SemaphoreType.DMA],
        compiler_params=params(63, collective_id=1, has_side_effects=True),
        name='finish',
    )(grads, mask, partial, picked, masks, lse_sum)


def solution(mesh):
    dp_size, vp = mesh.shape['dp'], mesh.shape['vp']

    def local_step(hidden, norm_gain, emb_table, labels, tok_mask):
        rows, seq_len, width = hidden.shape
        vocab = emb_table.shape[0]
        tokens = rows * seq_len
        blocks = tokens // TB
        share = tokens // vp
        my_vp = lax.axis_index('vp')
        my_dp = lax.axis_index('dp')
        gain = norm_gain.reshape(1, width)
        n_own, piece, compact, meta, nb_own = prologue(
            hidden.reshape(tokens, width), gain, labels, tok_mask, vp)
        pieces = lax.all_gather(piece, ('dp', 'vp'), axis=0)
        z, st_own = pass_one(nb_own, jnp.zeros((1,), jnp.int32), n_own, emb_table, None, 0, blocks)
        meta_oth = lax.dynamic_slice(pieces, ((1 - my_dp) * vp, share, 0), (1, 2, tokens))[0]
        nb_oth = lax.div(jnp.sum(meta_oth[1]).astype(jnp.int32) + (TB - 1), TB)[None]
        z, st_oth, n_oth = pass_one(nb_oth, (1 - my_dp)[None], pieces, emb_table, z, blocks, blocks)
        n_own, n_oth = n_own.reshape(blocks, TB, width), n_oth.reshape(blocks, TB, width)
        mask_own, mask_oth = meta[1].reshape(blocks, TB), meta_oth[1].reshape(blocks, TB)
        tokf, lse_sum = combine_stats(st_own, st_oth, mask_own, mask_oth, vp)
        ids = jnp.concatenate([meta[0], meta_oth[0]]).astype(jnp.int32).reshape(2 * blocks, 1, TB) - my_vp * vocab
        toki = jnp.where((ids >= 0) & (ids < vocab), ids, -vocab)
        dz_own, d_part, picked = pass_two_own(nb_own, tokf, toki, emb_table, z, blocks)
        d_share = lax.psum_scatter(d_part.reshape(tokens, width), 'vp', scatter_dimension=0, tiled=True)
        args = (nb_own, nb_oth, tokf, toki, n_own, n_oth, dz_own, z)
        steps, cut = -(-vocab // 1280), SPLIT
        d_table, picked_a = pass_two_table(*args, None, None, 0, cut)
        grads, gain_part = norm_back(d_share, compact, gain, picked_a)
        d_table, picked_b = pass_two_table(*args, d_table, gain_part, cut, steps)
        all_grads = lax.all_gather(grads, 'vp', axis=0, tiled=True)
        d_hidden, d_gain, loss = finish(
            all_grads, tok_mask, gain_part, jnp.concatenate([picked, picked_a + picked_b]),
            jnp.concatenate([mask_own, mask_oth]), lse_sum, dp_size, vp)
        return loss[0, 0], d_table, d_hidden.reshape(rows, seq_len, width), d_gain.reshape(width)

    return jax.shard_map(
        local_step, mesh=mesh,
        in_specs=(P('dp', None, None), P(None), P('vp', None), P('dp', None), P('dp', None)),
        out_specs=(P(), P('vp', None), P('dp', None, None), P(None)), check_vma=False)
```
